32 devices in a mesh: tx: 8 (over y, x, core), ty: 4 (over z).
Axes of the slice: x: 2, y: 2, z: 4, core: 2. Of those that a mesh axis runs over, the one named last changes fastest.
Arguments:
- mag: float32 [3, 2048, 2048], P(None, 'tx', 'ty'), may hold values from -1 to 1, as said below
- occupancy: int32 [2048, 2048], P('tx', 'ty'), may hold values from 0 to 1
- kernel_spectrum: float32 [4, 4096, 4096], P(None, ('tx', 'ty')), may hold values from -0.5 to 1, as said below
Outputs:
- mag_next: float32 [3, 2048, 2048], P(None, 'tx', 'ty')
- mean_rate: float32 [3, 2048, 2048], P(None, 'tx', 'ty')
The draws below stay inside these ranges and needn't reach their ends.
Inputs may be any that keep to these rules, and one draw needn't show every extreme that they name: `mag`: each cell's three components have unit length. `kernel_spectrum`: each component is unchanged under (y frequency, x frequency) -> ((4096 - y frequency) mod 2 * 2048, (4096 - x frequency) mod 2 * 2048).
All inputs are finite; a program needn't handle non-finite values.
Results may differ from the reference program's by a relative error of at most 0.00005.
Values sent between devices are 32-bit elements; how exact they have to be, the bound alone decides.
No kernel may reach another device: no remote copies, remote signals or barrier semaphores. Data moves between devices by JAX's collectives and lax.ppermute only.
A program may use at most 192 MiB of HBM per device.

```python
import jax
import jax.numpy as jnp
from jax import lax

NX = 2048
NY = 2048
N_TX = 8
N_TY = 4


def draw_mag(key, part):
    raw = jax.random.normal(key, (3, NX, NY), jnp.float32)
    return raw / jnp.sqrt(jnp.sum(raw * raw, axis=0, keepdims=True) + 1e-12)


def draw_occupancy(key, part):
    block_key, cell_key = jax.random.split(jax.random.fold_in(key, 7))
    block_rows = NX // 8
    block_cols = NY // 8
    levels = jax.random.randint(block_key, (block_rows, block_cols), 0, 8)
    limits = 5 + 3 * jnp.arange(block_rows, dtype=jnp.int32) // max(block_rows - 1, 1)
    blocks = (levels < limits[:, None]).astype(jnp.int32)
    cells = (jax.random.randint(cell_key, (NX, NY), 0, 8) != 0).astype(jnp.int32)
    pattern = jnp.repeat(jnp.repeat(blocks, 8, axis=0), 8, axis=1) * cells
    row_band = jnp.arange(NX, dtype=jnp.int32) % (NX // N_TX) < 8
    col_band = jnp.arange(NY, dtype=jnp.int32) % (NY // N_TY) < 8
    band = jnp.logical_or(row_band[:, None], col_band[None, :]).astype(jnp.int32)
    return jnp.maximum(pattern, band)


def draw_kernel_spectrum(key, part):
    raw = jax.random.uniform(jax.random.fold_in(key, 11), (4, 2 * NY, 2 * NX), jnp.float32, -0.5, 1.0)
    mirror = jnp.roll(jnp.flip(raw, axis=(1, 2)), 1, axis=(1, 2))
    return 0.5 * (raw + mirror)


def setup_inputs(seed: int = 0) -> dict:
    key_list = jax.random.split(jax.random.key(seed), 4)
    return {
        "mag": draw_mag(jax.random.fold_in(key_list[3], 71), 0),
        "occupancy": draw_occupancy(jax.random.fold_in(key_list[3], 71), 0),
        "kernel_spectrum": draw_kernel_spectrum(jax.random.fold_in(key_list[3], 71), 0),
    }


DAMPING = 0.3
STIFFNESS = 0.25
TIME_STEP = 0.25

def neighbours(field):
    padded = jnp.pad(field, ((0, 0), (1, 1), (1, 1)))
    return padded[:, 2:, 1:-1] + padded[:, :-2, 1:-1] + padded[:, 1:-1, 2:] + padded[:, 1:-1, :-2]

def cross(left, right):
    return jnp.stack([left[1] * right[2] - left[2] * right[1], left[2] * right[0] - left[0] * right[2], left[0] * right[1] - left[1] * right[0]])

def demag(field, kernel_spectrum):
    padded = jnp.zeros((3, 2 * NX, 2 * NY), field.dtype).at[:, :NX, :NY].set(field)
    spectrum = jnp.fft.fft2(padded)
    kernel = jnp.transpose(kernel_spectrum, (0, 2, 1))
    field_x = -(kernel[0] * spectrum[0] + kernel[3] * spectrum[1])
    field_y = -(kernel[3] * spectrum[0] + kernel[1] * spectrum[1])
    field_z = -(kernel[2] * spectrum[2])
    back = jnp.fft.ifft2(jnp.stack([field_x, field_y, field_z])).real
    return back[:, :NX, :NY].astype(field.dtype)

def reference(mag, occupancy, kernel_spectrum):
    occ = occupancy.astype(jnp.float32)
    start = mag * occ[None]

    def rate(field):
        effective = demag(field, kernel_spectrum) + STIFFNESS * neighbours(field)
        torque = cross(field, effective)
        return -(torque + DAMPING * cross(field, torque)) / (1.0 + DAMPING * DAMPING)

    def normal(vector):
        return vector / jnp.sqrt(lax.optimization_barrier(jnp.sum(vector * vector, axis=0)) + 1.0 - occ)[None]
    first = rate(start)
    middle = normal(start + TIME_STEP * first)
    second = rate(middle)
    second = second - lax.optimization_barrier(jnp.sum(second * start, axis=0))[None] * start
    mean_rate = 0.5 * (first + second)
    mag_next = normal(start + TIME_STEP * mean_rate)
    return (mag_next, mean_rate)
```

```python
import functools
import math

import jax
import jax.numpy as jnp
import numpy as np
from jax import lax
from jax.experimental import pallas as pl
from jax.experimental.pallas import tpu as pltpu
from jax.sharding import PartitionSpec as P

DAMPING = 0.3
STIFFNESS = 0.25
TIME_STEP = 0.25
LANES = 128
AXES = ("tx", "ty")


def halves(values):
    high = values.astype(jnp.bfloat16)
    low = (values - high.astype(jnp.float32)).astype(jnp.bfloat16)
    return high, low


def np_halves(values):
    values = np.asarray(values, np.float64)
    high = values.astype(np.float32).astype(jnp.bfloat16)
    low = (values - high.astype(np.float64)).astype(np.float32).astype(jnp.bfloat16)
    return jnp.asarray(high), jnp.asarray(low)


def dot(left, right, dims):
    return lax.dot_general(left, right, (dims, ((), ())), preferred_element_type=jnp.float32)


def dot_3(left, right, dims=((1,), (0,))):
    return (
        dot(left[0], right[0], dims) + dot(left[1], right[0], dims) + dot(left[0], right[1], dims)
    )


NT = ((1,), (1,))


def c_add(a, b):
    if a is None:
        return b
    if b is None:
        return a
    re = a[0] + b[0]
    if a[1] is None or b[1] is None:
        return (re, b[1] if a[1] is None else a[1])
    return (re, a[1] + b[1])


def c_sub(a, b):
    if b is None:
        return a
    re = a[0] - b[0]
    if b[1] is None:
        return (re, a[1])
    return (re, -b[1] if a[1] is None else a[1] - b[1])


def c_turn(a, num, den, sign):
    num %= den
    if a is None or num == 0:
        return a
    re, im = a
    if 4 * num == den:
        return (None, sign * re) if im is None else (-sign * im, sign * re)
    cos, sin = math.cos(2 * math.pi * num / den), sign * math.sin(2 * math.pi * num / den)
    if im is None:
        return (re * cos, re * sin)
    return (re * cos - im * sin, re * sin + im * cos)


def fix(a):
    if a is not None and a[0] is None:
        return (jnp.zeros_like(a[1]), a[1])
    return a


def fft(items, sign, wanted):
    size = len(items)
    if size == 1:
        return {0: items[0]}
    half = size // 2
    result = {}
    even = sorted({k // 2 for k in wanted if k % 2 == 0})
    odd = sorted({k // 2 for k in wanted if k % 2 == 1})
    if even:
        sub = fft([c_add(items[i], items[i + half]) for i in range(half)], sign, even)
        result.update({2 * k: v for k, v in sub.items()})
    if odd:
        parts = [
            fix(c_turn(c_sub(items[i], items[i + half]), i, size, sign)) for i in range(half)
        ]
        result.update({2 * k + 1: v for k, v in fft(parts, sign, odd).items()})
    return result


class Plan:
    def __init__(self, mag_shape, n_tx, n_ty):
        self.n_ty = n_ty
        self.devices = n = n_tx * n_ty
        self.block_x, self.block_y = mag_shape[1:]
        self.rows = self.block_x // n_ty
        self.len_x, self.len_y = 2 * self.block_x * n_tx, 2 * self.block_y * n_ty
        self.slots = self.len_y // 2 // LANES
        self.residues = 2 * self.slots
        self.near = self.len_y // n // self.residues
        self.group = LANES // self.rows
        self.steps = self.slots // self.group
        self.freq = n * 2 * self.near
        self.spread = 2 * n * self.near

    def y_tables(self):
        k1 = np.arange(LANES)
        spot = np.arange(LANES)
        angle = 2 * np.pi * np.outer(k1, spot) / LANES
        cos, sin = np.cos(angle), np.sin(angle)

        def rows(re_re, re_im, im_re, im_im):
            full = np.stack(
                [np.concatenate([re_re, re_im], 1), np.concatenate([im_re, im_im], 1)]
            )
            full = full.reshape(2, self.devices, self.near, 2 * LANES)
            return full.transpose(1, 0, 2, 3).reshape(self.freq, 2 * LANES)

        plain = rows(cos, sin, -sin, cos)
        mixed = rows(-sin, cos, -cos, -sin)
        slot = np.arange(self.slots)
        turn = 2 * np.pi * np.outer(slot, spot) / self.len_y
        turn_cos = np.tile(np.cos(turn), 2).reshape(self.steps, 1, self.group * 2 * LANES)
        turn_sin = np.tile(np.sin(turn), 2).reshape(self.steps, 1, self.group * 2 * LANES)
        late = 2 * np.pi * np.outer(k1 + 0.5, spot) / LANES
        low = (k1 < LANES // 2)[:, None]
        zero = np.zeros_like(cos)
        im_first = np.where(low, -sin, 0)
        im_first[0] = np.cos(np.pi * spot)
        first = rows(
            np.where(low, cos, zero),
            np.where(low, zero, np.cos(late)),
            im_first,
            np.where(low, zero, -np.sin(late)),
        )
        return plain, mixed, turn_cos, turn_sin, first

    def y_matrices(self):
        plain, mixed, turn_cos, turn_sin, first = (
            jnp.asarray(t, jnp.float32) for t in self.y_tables()
        )
        plain = jnp.concatenate([plain] * self.group, axis=1)[None]
        mixed = jnp.concatenate([mixed] * self.group, axis=1)[None]
        full = plain * turn_cos + mixed * turn_sin
        first = jnp.pad(first, ((0, 0), (0, (self.group - 1) * 2 * LANES)))[None]
        shape = (self.steps, 1, self.group * 2 * LANES)
        at_first = (lax.broadcasted_iota(jnp.int32, shape, 0) == 0) & (
            lax.broadcasted_iota(jnp.int32, shape, 2) < 2 * LANES
        )
        return jnp.where(at_first, first, full)

    def x_first(self):
        n = self.devices
        angle = 2 * np.pi * np.outer(np.arange(2 * n), np.arange(n)) / (2 * n)
        cos, sin = np.cos(angle), np.sin(angle)
        table = np.stack([np.stack([cos, sin], -1), np.stack([-sin, cos], -1)])
        full = np.einsum("orsi,fg->orfsig", table, np.eye(self.near))
        return full.reshape(2 * self.spread, self.freq)

    def x_turn(self):
        angle = -2 * np.pi * np.outer(np.arange(2 * self.devices), np.arange(self.rows))
        angle = np.repeat(angle / self.len_x, self.near, axis=0)
        angle = np.tile(angle, (1, self.group))
        return np.stack([np.cos(angle), np.sin(angle)]).astype(np.float32)

    def x_second(self):
        span = np.arange(self.rows)
        angle = 2 * np.pi * np.outer(span, span) / self.rows
        cos, sin = np.cos(angle), np.sin(angle)
        table = np.stack([np.stack([cos, -sin], 1), np.stack([sin, cos], 1)])
        full = np.einsum("ixok,qp->iqxopk", table, np.eye(self.group))
        return full.reshape(2 * LANES, 2 * LANES)


def y_forward_kernel(plan, rows_ref, high_ref, low_ref, out_ref, z_high, z_low):
    step = pl.program_id(0)
    chunk = 16
    per = plan.rows // chunk
    blocks = plan.block_y // LANES

    @pl.when(step == 0)
    def _():
        if plan.group > 1:
            z_high[...] = jnp.zeros_like(z_high)
            z_low[...] = jnp.zeros_like(z_low)

        def one(index, carry):
            comp = index // per
            start = pl.multiple_of((index % per) * chunk, chunk)
            items = []
            for block in range(plan.slots):
                lane = block % blocks * LANES
                items.append(
                    (
                        rows_ref[
                            block // blocks, comp, pl.ds(start, chunk), lane : lane + LANES
                        ],
                        None,
                    )
                )
            items += [None] * plan.slots
            parts = fft(items, -1, list(range(plan.slots + 1)))
            for slot in range(plan.slots):
                pair = (parts[0][0], parts[plan.slots][0]) if slot == 0 else parts[slot]
                place, inner = slot // plan.group, slot % plan.group
                row = pl.multiple_of(comp * LANES + inner * plan.rows + start, chunk)
                for half in range(2):
                    lane = inner * 2 * LANES + half * LANES
                    high, low = halves(pair[half])
                    z_high[place, pl.ds(row, chunk), lane : lane + LANES] = high
                    z_low[place, pl.ds(row, chunk), lane : lane + LANES] = low
            return carry

        lax.fori_loop(0, 3 * per, one, 0)

    left = (high_ref[0], low_ref[0])
    out_ref[...] = dot_3(left, (z_high[step], z_low[step]), NT)


def y_forward(plan, rows, high, low):
    wide = 3 * LANES
    deep = plan.group * 2 * LANES
    matrix = pl.BlockSpec((1, plan.freq, deep), lambda i: (i, 0, 0))
    return pl.pallas_call(
        functools.partial(y_forward_kernel, plan),
        grid=(plan.steps,),
        in_specs=[
            pl.BlockSpec(rows.shape, lambda i: (0, 0, 0, 0)),
            matrix,
            matrix,
        ],
        out_specs=pl.BlockSpec((plan.freq, wide), lambda i: (0, i)),
        out_shape=jax.ShapeDtypeStruct((plan.freq, wide * plan.steps), jnp.float32),
        scratch_shapes=[
            pltpu.VMEM((plan.steps, wide, deep), jnp.bfloat16),
            pltpu.VMEM((plan.steps, wide, deep), jnp.bfloat16),
        ],
        compiler_params=pltpu.CompilerParams(vmem_limit_bytes=50 * 2**20),
        cost_estimate=pl.CostEstimate(
            flops=6 * plan.freq * wide * plan.steps * deep,
            bytes_accessed=10 * 2**20,
            transcendentals=0,
        ),
        name="y_forward",
    )(rows, high, low)


def x_kernel(
    plan,
    data_ref,
    gain_ref,
    shift_ref,
    mirror_ref,
    one_high,
    one_low,
    back_high,
    back_low,
    two_high,
    two_low,
    turn_ref,
    out_ref,
    field_ref,
):
    one = (one_high[...], one_low[...])
    two = (two_high[...], two_low[...])
    turn_re, turn_im = turn_ref[0], turn_ref[1]
    size = plan.spread

    def cut(comp):
        return slice(comp * LANES, (comp + 1) * LANES)

    def spectrum(data):
        section = dot_3(one, halves(data))
        result = []
        for comp in range(3):
            re, im = section[:size, cut(comp)], section[size:, cut(comp)]
            turned = jnp.concatenate(
                [re * turn_re - im * turn_im, re * turn_im + im * turn_re], axis=1
            )
            result.append(dot_3(halves(turned), two))
        return result

    def apply(gain, parts):
        result = []
        for comp in range(3):
            wide = [jnp.concatenate([gain(i)] * 2, axis=1) for i in ((0, 3), (3, 1), (2,))[comp]]
            if comp == 2:
                result.append(wide[0] * parts[2])
            else:
                result.append(wide[0] * parts[0] + wide[1] * parts[1])
        return result

    data = data_ref[...]
    parts = spectrum(data)
    for comp, value in enumerate(apply(lambda i: gain_ref[i, 0], parts)):
        field_ref[comp] = value

    @pl.when(pl.program_id(0) == 0)
    def _():
        row = lax.broadcasted_iota(jnp.int32, (plan.freq, 1), 0)
        sign = jnp.where(row // plan.near % 2 == 0, 1.0, -1.0)
        other = spectrum(data * sign)
        added = apply(lambda i: shift_ref[i], parts)
        flipped = apply(lambda i: mirror_ref[i], other)
        for comp in range(3):
            field_ref[comp] += added[comp] + flipped[comp]

    re_list, im_list = [], []
    for comp in range(3):
        value = dot_3(halves(field_ref[comp]), two, NT)
        re, im = value[:, :LANES], value[:, LANES:]
        re_list.append(re * turn_re + im * turn_im)
        im_list.append(im * turn_re - re * turn_im)
    section = jnp.concatenate(
        [jnp.concatenate(re_list, axis=1), jnp.concatenate(im_list, axis=1)], axis=0
    )
    out_ref[...] = dot_3((back_high[...], back_low[...]), halves(section))


def x_stage(plan, data, gains, tables):
    gain, shift, mirror = gains
    wide = 3 * LANES
    lane_block = pl.BlockSpec((plan.freq, wide), lambda i: (0, i))

    def whole(array):
        return pl.BlockSpec(array.shape, lambda i: (0,) * array.ndim)

    return pl.pallas_call(
        functools.partial(x_kernel, plan),
        grid=(plan.steps,),
        in_specs=[
            lane_block,
            pl.BlockSpec((4, 1, plan.spread, LANES), lambda i: (0, i, 0, 0)),
            whole(shift),
            whole(mirror),
            *[whole(t) for t in tables],
        ],
        out_specs=lane_block,
        out_shape=jax.ShapeDtypeStruct(data.shape, jnp.float32),
        scratch_shapes=[pltpu.VMEM((3, plan.spread, 2 * LANES), jnp.float32)],
        compiler_params=pltpu.CompilerParams(vmem_limit_bytes=50 * 2**20),
        cost_estimate=pl.CostEstimate(
            flops=24 * plan.freq * wide * plan.steps * 2 * plan.spread,
            bytes_accessed=12 * 2**20,
            transcendentals=0,
        ),
        name="x_stage",
    )(data, gain, shift, mirror, *tables)


def y_inverse_kernel(plan, data_ref, high_ref, low_ref, turn_ref, out_ref, inner_ref, sum_ref):
    step = pl.program_id(0)
    value = dot_3((high_ref[0], low_ref[0]), halves(data_ref[...]))
    deep = 2 * LANES
    lane = lax.broadcasted_iota(jnp.int32, (1, LANES), 1)
    for comp in range(3):
        mixed = value[:deep, comp * LANES : (comp + 1) * LANES]
        for inner in range(1, plan.group):
            mixed = jnp.where(
                lane // plan.rows == inner,
                value[inner * deep : (inner + 1) * deep, comp * LANES : (comp + 1) * LANES],
                mixed,
            )
        inner_ref[comp, step] = mixed

    @pl.when(step == plan.steps - 1)
    def _():
        chunk = 8
        blocks = plan.block_y // LANES

        def one_comp(comp, carry):
            def one(index, carry):
                start = pl.multiple_of(index * chunk, chunk)
                items = [
                    (
                        inner_ref[comp, place, pl.ds(start, chunk), :],
                        inner_ref[comp, place, pl.ds(LANES + start, chunk), :],
                    )
                    for place in range(plan.steps)
                ]
                odd = jnp.where(lane < plan.rows, items[0][1], 0.0)
                period = 2 * plan.steps
                parts = fft(items + [None] * plan.steps, 1, list(range(period)))
                for block in range(plan.slots):
                    re, im = parts[block % period]
                    total = re * turn_ref[0, block : block + 1, :]
                    total = total - im * turn_ref[1, block : block + 1, :]
                    total = total + odd if block % 2 == 0 else total - odd
                    shift = LANES // 2
                    while shift >= plan.rows:
                        total = total + pltpu.roll(total, shift, 1)
                        shift //= 2
                    sum_ref[block, pl.ds(start, chunk), :] = total
                return carry

            lax.fori_loop(0, LANES // chunk, one, 0)
            for block in range(plan.slots):
                first = block % blocks * LANES
                out_ref[block // blocks, comp, :, first : first + LANES] = sum_ref[block].T[
                    : plan.rows
                ]
            return carry

        lax.fori_loop(0, 3, one_comp, 0)


def y_inverse(plan, data, high, low):
    wide = 3 * LANES
    deep = plan.group * 2 * LANES
    matrix = pl.BlockSpec((1, deep, plan.freq), lambda i: (i, 0, 0))
    shape = (plan.n_ty, 3, plan.rows, plan.block_y)
    inner = np.arange(LANES) // plan.rows
    angle = 2 * np.pi * np.outer(np.arange(plan.slots), inner) / plan.residues
    turn = jnp.asarray(np.stack([np.cos(angle), np.sin(angle)]), jnp.float32)
    return pl.pallas_call(
        functools.partial(y_inverse_kernel, plan),
        grid=(plan.steps,),
        in_specs=[
            pl.BlockSpec((plan.freq, wide), lambda i: (0, i)),
            matrix,
            matrix,
            pl.BlockSpec(turn.shape, lambda i: (0, 0, 0)),
        ],
        out_specs=pl.BlockSpec(shape, lambda i: (0, 0, 0, 0)),
        out_shape=jax.ShapeDtypeStruct(shape, jnp.float32),
        scratch_shapes=[
            pltpu.VMEM((3, plan.steps, 2 * LANES, LANES), jnp.float32),
            pltpu.VMEM((plan.slots, LANES, LANES), jnp.float32),
        ],
        compiler_params=pltpu.CompilerParams(vmem_limit_bytes=50 * 2**20),
        cost_estimate=pl.CostEstimate(
            flops=6 * plan.freq * wide * plan.steps * deep,
            bytes_accessed=10 * 2**20,
            transcendentals=0,
        ),
        name="y_inverse",
    )(data, high, low, turn)


def kernel_gains(plan, kernel):
    n, near, slots = plan.devices, plan.near, plan.slots
    me = lax.axis_index(AXES)
    scale = 2.0 / (plan.len_x * plan.len_y)
    kx = np.arange(plan.len_x)
    wave_x = jnp.asarray(2 * STIFFNESS * np.cos(2 * np.pi * kx / plan.len_x), jnp.float32)
    diagonal = jnp.asarray([1.0, 1.0, 1.0, 0.0], jnp.float32)

    nyquist = lax.ppermute(kernel[:, 0, :], AXES, [(n // 2, 0)])
    split = kernel.reshape(4, near, plan.residues, plan.len_x)
    first = jnp.where(me < n // 2, split[:, :, :1], split[:, :, slots : slots + 1])
    chosen = jnp.concatenate([first, split[:, :, 1:slots]], axis=2)
    slot = lax.broadcasted_iota(jnp.int32, (near, slots), 1)
    slot = jnp.where((slot == 0) & (me >= n // 2), slots, slot)
    ky = (me * near + lax.broadcasted_iota(jnp.int32, (near, slots), 0)) * plan.residues + slot
    wave_y = 2 * STIFFNESS * jnp.cos(ky.astype(jnp.float32) * (2 * math.pi / plan.len_y))
    wave = wave_x[None, None, :] + wave_y[:, :, None]
    gain = (diagonal[:, None, None, None] * wave[None] - chosen) * scale

    def arrange(array, count_near, count_slots):
        group = min(plan.group, count_slots)
        shaped = array.reshape(4, count_near, count_slots // group, group, plan.rows, 2 * n)
        moved = shaped.transpose(0, 2, 5, 1, 3, 4)
        return moved.reshape(4, count_slots // group, 2 * n * count_near, group * plan.rows)

    zero_row = (diagonal[:, None] * (wave_x + 2 * STIFFNESS)[None] - kernel[:, 0, :]) * scale
    last_row = (diagonal[:, None] * (wave_x - 2 * STIFFNESS)[None] - nyquist) * scale
    shift = jnp.where(me == 0, 0.25 * (zero_row + last_row) - zero_row, 0.0)
    mirror = jnp.where(me == 0, 0.25 * (zero_row - last_row), 0.0)

    def place(row):
        small = row.reshape(4, plan.rows, 2 * n).transpose(0, 2, 1)[:, :, None, :]
        small = jnp.pad(small, ((0, 0), (0, 0), (0, near - 1), (0, LANES - plan.rows)))
        return small.reshape(4, plan.spread, LANES)

    return arrange(gain, near, slots), place(shift), place(mirror)


def cross(left, right):
    return jnp.stack(
        [
            left[1] * right[2] - left[2] * right[1],
            left[2] * right[0] - left[0] * right[2],
            left[0] * right[1] - left[1] * right[0],
        ]
    )


def exchange(values, axes):
    return lax.all_to_all(values, axes, split_axis=0, concat_axis=0, tiled=True)


def body(mag, occupancy, kernel_spectrum):
    plan = Plan(mag.shape, lax.axis_size("tx"), lax.axis_size("ty"))
    occ = occupancy.astype(jnp.float32)
    start = mag * occ[None]
    matrix = plan.y_matrices()
    rounded = lax.reduce_precision(matrix, 8, 7)
    high, low = rounded.astype(jnp.bfloat16), (matrix - rounded).astype(jnp.bfloat16)
    high_back, low_back = jnp.swapaxes(high, 1, 2), jnp.swapaxes(low, 1, 2)
    one = plan.x_first()
    tables = (
        *np_halves(one),
        *np_halves(one.T),
        *np_halves(plan.x_second()),
        jnp.asarray(plan.x_turn()),
    )
    gains = kernel_gains(plan, kernel_spectrum)
    sent_shape = (plan.devices, 2 * plan.near, 3 * plan.slots * plan.rows)
    flat_shape = (plan.freq, sent_shape[2])

    def effective(field):
        shaped = field.reshape(3, plan.n_ty, plan.rows, plan.block_y).transpose(1, 0, 2, 3)
        rows = exchange(shaped, "ty")
        spectra = y_forward(plan, rows, high, low)
        columns = exchange(spectra.reshape(sent_shape), AXES).reshape(flat_shape)
        product = x_stage(plan, columns, gains, tables)
        returned = exchange(product.reshape(sent_shape), AXES).reshape(flat_shape)
        spatial = exchange(y_inverse(plan, returned, high_back, low_back), "ty")
        return spatial.transpose(1, 0, 2, 3).reshape(field.shape)

    def rate(field):
        torque = cross(field, effective(field))
        return -(torque + DAMPING * cross(field, torque)) / (1.0 + DAMPING * DAMPING)

    def normal(vector):
        return vector / jnp.sqrt(jnp.sum(vector * vector, axis=0) + 1.0 - occ)[None]

    first = rate(start)
    middle = normal(start + TIME_STEP * first)
    second = rate(middle)
    second = second - jnp.sum(second * start, axis=0)[None] * start
    mean_rate = 0.5 * (first + second)
    mag_next = normal(start + TIME_STEP * mean_rate)
    return (mag_next, mean_rate)


def solution(mesh):
    return jax.shard_map(
        body,
        mesh=mesh,
        in_specs=(P(None, "tx", "ty"), P("tx", "ty"), P(None, ("tx", "ty"), None)),
        out_specs=(P(None, "tx", "ty"), P(None, "tx", "ty")),
        check_vma=False,
    )
```

```python
import functools
import math

import jax
import jax.numpy as jnp
import numpy as np
from jax import lax
from jax.experimental import pallas as pl
from jax.experimental.pallas import tpu as pltpu
from jax.sharding import PartitionSpec as P

DAMPING = 0.3
STIFFNESS = 0.25
TIME_STEP = 0.25
LANES = 128
AXES = ("tx", "ty")


def halves(values):
    high = values.astype(jnp.bfloat16)
    low = (values - high.astype(jnp.float32)).astype(jnp.bfloat16)
    return high, low


def np_halves(values):
    values = np.asarray(values, np.float64)
    high = values.astype(np.float32).astype(jnp.bfloat16)
    low = (values - high.astype(np.float64)).astype(np.float32).astype(jnp.bfloat16)
    return jnp.asarray(high), jnp.asarray(low)


def dot(left, right, dims):
    return lax.dot_general(left, right, (dims, ((), ())), preferred_element_type=jnp.float32)


def dot_3(left, right, dims=((1,), (0,))):
    return (
        dot(left[0], right[0], dims) + dot(left[1], right[0], dims) + dot(left[0], right[1], dims)
    )


NT = ((1,), (1,))


def c_add(a, b):
    if a is None:
        return b
    if b is None:
        return a
    re = a[0] + b[0]
    if a[1] is None or b[1] is None:
        return (re, b[1] if a[1] is None else a[1])
    return (re, a[1] + b[1])


def c_sub(a, b):
    if b is None:
        return a
    re = a[0] - b[0]
    if b[1] is None:
        return (re, a[1])
    return (re, -b[1] if a[1] is None else a[1] - b[1])


def c_turn(a, num, den, sign):
    num %= den
    if a is None or num == 0:
        return a
    re, im = a
    if 4 * num == den:
        return (None, sign * re) if im is None else (-sign * im, sign * re)
    cos, sin = math.cos(2 * math.pi * num / den), sign * math.sin(2 * math.pi * num / den)
    if im is None:
        return (re * cos, re * sin)
    return (re * cos - im * sin, re * sin + im * cos)


def fix(a):
    if a is not None and a[0] is None:
        return (jnp.zeros_like(a[1]), a[1])
    return a


def fft(items, sign, wanted):
    size = len(items)
    if size == 1:
        return {0: items[0]}
    half = size // 2
    result = {}
    even = sorted({k // 2 for k in wanted if k % 2 == 0})
    odd = sorted({k // 2 for k in wanted if k % 2 == 1})
    if even:
        sub = fft([c_add(items[i], items[i + half]) for i in range(half)], sign, even)
        result.update({2 * k: v for k, v in sub.items()})
    if odd:
        parts = [
            fix(c_turn(c_sub(items[i], items[i + half]), i, size, sign)) for i in range(half)
        ]
        result.update({2 * k + 1: v for k, v in fft(parts, sign, odd).items()})
    return result


class Plan:
    def __init__(self, mag_shape, n_tx, n_ty):
        self.n_ty = n_ty
        self.devices = n = n_tx * n_ty
        self.block_x, self.block_y = mag_shape[1:]
        self.rows = self.block_x // n_ty
        self.len_x, self.len_y = 2 * self.block_x * n_tx, 2 * self.block_y * n_ty
        self.slots = self.len_y // 2 // LANES
        self.residues = 2 * self.slots
        self.near = self.len_y // n // self.residues
        self.group = LANES // self.rows
        self.steps = self.slots // self.group
        self.freq = n * 2 * self.near
        self.spread = 2 * n * self.near

    def y_tables(self):
        k1 = np.arange(LANES)
        spot = np.arange(LANES)
        angle = 2 * np.pi * np.outer(k1, spot) / LANES
        cos, sin = np.cos(angle), np.sin(angle)

        def rows(re_re, re_im, im_re, im_im):
            full = np.stack(
                [np.concatenate([re_re, re_im], 1), np.concatenate([im_re, im_im], 1)]
            )
            full = full.reshape(2, self.devices, self.near, 2 * LANES)
            return full.transpose(1, 0, 2, 3).reshape(self.freq, 2 * LANES)

        plain = rows(cos, sin, -sin, cos)
        mixed = rows(-sin, cos, -cos, -sin)
        slot = np.arange(self.slots)
        turn = 2 * np.pi * np.outer(slot, spot) / self.len_y
        turn_cos = np.tile(np.cos(turn), 2).reshape(self.steps, 1, self.group * 2 * LANES)
        turn_sin = np.tile(np.sin(turn), 2).reshape(self.steps, 1, self.group * 2 * LANES)
        late = 2 * np.pi * np.outer(k1 + 0.5, spot) / LANES
        low = (k1 < LANES // 2)[:, None]
        zero = np.zeros_like(cos)
        im_first = np.where(low, -sin, 0)
        im_first[0] = np.cos(np.pi * spot)
        first = rows(
            np.where(low, cos, zero),
            np.where(low, zero, np.cos(late)),
            im_first,
            np.where(low, zero, -np.sin(late)),
        )
        return plain, mixed, turn_cos, turn_sin, first

    def y_matrices(self):
        plain, mixed, turn_cos, turn_sin, first = (
            jnp.asarray(t, jnp.float32) for t in self.y_tables()
        )
        plain = jnp.concatenate([plain] * self.group, axis=1)[None]
        mixed = jnp.concatenate([mixed] * self.group, axis=1)[None]
        full = plain * turn_cos + mixed * turn_sin
        first = jnp.pad(first, ((0, 0), (0, (self.group - 1) * 2 * LANES)))[None]
        shape = (self.steps, 1, self.group * 2 * LANES)
        at_first = (lax.broadcasted_iota(jnp.int32, shape, 0) == 0) & (
            lax.broadcasted_iota(jnp.int32, shape, 2) < 2 * LANES
        )
        return jnp.where(at_first, first, full)

    def x_first(self):
        n = self.devices
        angle = 2 * np.pi * np.outer(np.arange(2 * n), np.arange(n)) / (2 * n)
        cos, sin = np.cos(angle), np.sin(angle)
        table = np.stack([np.stack([cos, sin], -1), np.stack([-sin, cos], -1)])
        full = np.einsum("orsi,fg->orfsig", table, np.eye(self.near))
        return full.reshape(2 * self.spread, self.freq)

    def x_turn(self):
        angle = -2 * np.pi * np.outer(np.arange(2 * self.devices), np.arange(self.rows))
        angle = np.repeat(angle / self.len_x, self.near, axis=0)
        angle = np.tile(angle, (1, self.group))
        return np.stack([np.cos(angle), np.sin(angle)]).astype(np.float32)

    def x_second(self):
        span = np.arange(self.rows)
        angle = 2 * np.pi * np.outer(span, span) / self.rows
        cos, sin = np.cos(angle), np.sin(angle)
        table = np.stack([np.stack([cos, -sin], 1), np.stack([sin, cos], 1)])
        full = np.einsum("ixok,qp->iqxopk", table, np.eye(self.group))
        return full.reshape(2 * LANES, 2 * LANES)


def y_forward_kernel(plan, place_ref, rows_ref, high_ref, low_ref, out_ref, z_high, z_low):
    step = pl.program_id(0)
    chunk = 16
    per = plan.rows // chunk
    blocks = plan.block_y // LANES

    @pl.when(step == 0)
    def _():
        if plan.group > 1:
            z_high[...] = jnp.zeros_like(z_high)
            z_low[...] = jnp.zeros_like(z_low)

        def one(index, carry):
            comp = index // per
            start = pl.multiple_of((index % per) * chunk, chunk)
            items = []
            for block in range(plan.slots):
                lane = block % blocks * LANES
                items.append(
                    (
                        rows_ref[
                            lax.bitwise_xor(block // blocks, place_ref[0]),
                            comp,
                            pl.ds(start, chunk),
                            lane : lane + LANES,
                        ],
                        None,
                    )
                )
            items += [None] * plan.slots
            parts = fft(items, -1, list(range(plan.slots + 1)))
            for slot in range(plan.slots):
                pair = (parts[0][0], parts[plan.slots][0]) if slot == 0 else parts[slot]
                place, inner = slot // plan.group, slot % plan.group
                row = pl.multiple_of(comp * LANES + inner * plan.rows + start, chunk)
                for half in range(2):
                    lane = inner * 2 * LANES + half * LANES
                    high, low = halves(pair[half])
                    z_high[place, pl.ds(row, chunk), lane : lane + LANES] = high
                    z_low[place, pl.ds(row, chunk), lane : lane + LANES] = low
            return carry

        lax.fori_loop(0, rows_ref.shape[1] * per, one, 0)

    left = (high_ref[0], low_ref[0])
    out_ref[...] = dot_3(left, (z_high[step], z_low[step]), NT)


def y_forward(plan, place, rows, high, low):
    wide = rows.shape[1] * LANES
    deep = plan.group * 2 * LANES
    matrix = pl.BlockSpec((1, plan.freq, deep), lambda i: (i, 0, 0))
    return pl.pallas_call(
        functools.partial(y_forward_kernel, plan),
        grid=(plan.steps,),
        in_specs=[
            pl.BlockSpec(memory_space=pltpu.SMEM),
            pl.BlockSpec(rows.shape, lambda i: (0, 0, 0, 0)),
            matrix,
            matrix,
        ],
        out_specs=pl.BlockSpec((plan.freq, wide), lambda i: (0, i)),
        out_shape=jax.ShapeDtypeStruct((plan.freq, wide * plan.steps), jnp.float32),
        scratch_shapes=[
            pltpu.VMEM((plan.steps, wide, deep), jnp.bfloat16),
            pltpu.VMEM((plan.steps, wide, deep), jnp.bfloat16),
        ],
        compiler_params=pltpu.CompilerParams(vmem_limit_bytes=50 * 2**20),
        cost_estimate=pl.CostEstimate(
            flops=6 * plan.freq * wide * plan.steps * deep,
            bytes_accessed=10 * 2**20,
            transcendentals=0,
        ),
        name="y_forward",
    )(place, rows, high, low)


def x_kernel(
    plan,
    data_ref,
    gain_ref,
    shift_ref,
    mirror_ref,
    one_high,
    one_low,
    back_high,
    back_low,
    two_high,
    two_low,
    turn_ref,
    out_ref,
    field_ref,
):
    one = (one_high[...], one_low[...])
    two = (two_high[...], two_low[...])
    turn_re, turn_im = turn_ref[0], turn_ref[1]
    size = plan.spread
    count = field_ref.shape[0]

    def cut(comp):
        return slice(comp * LANES, (comp + 1) * LANES)

    def spectrum(data):
        section = dot_3(one, halves(data))
        result = []
        for comp in range(count):
            re, im = section[:size, cut(comp)], section[size:, cut(comp)]
            turned = jnp.concatenate(
                [re * turn_re - im * turn_im, re * turn_im + im * turn_re], axis=1
            )
            result.append(dot_3(halves(turned), two))
        return result

    def apply(gain, parts):
        wide = [jnp.concatenate([gain(i)] * 2, axis=1) for i in range(2 * count - 1)]
        if count == 1:
            return [wide[0] * parts[0]]
        return [
            wide[0] * parts[0] + wide[2] * parts[1],
            wide[2] * parts[0] + wide[1] * parts[1],
        ]

    data = data_ref[...]
    parts = spectrum(data)
    for comp, value in enumerate(apply(lambda i: gain_ref[i, 0], parts)):
        field_ref[comp] = value

    @pl.when(pl.program_id(0) == 0)
    def _():
        row = lax.broadcasted_iota(jnp.int32, (plan.freq, 1), 0)
        sign = jnp.where(row // plan.near % 2 == 0, 1.0, -1.0)
        other = spectrum(data * sign)
        added = apply(lambda i: shift_ref[i], parts)
        flipped = apply(lambda i: mirror_ref[i], other)
        for comp in range(count):
            field_ref[comp] += added[comp] + flipped[comp]

    re_list, im_list = [], []
    for comp in range(count):
        value = dot_3(halves(field_ref[comp]), two, NT)
        re, im = value[:, :LANES], value[:, LANES:]
        re_list.append(re * turn_re + im * turn_im)
        im_list.append(im * turn_re - re * turn_im)
    section = jnp.concatenate(
        [jnp.concatenate(re_list, axis=1), jnp.concatenate(im_list, axis=1)], axis=0
    )
    out_ref[...] = dot_3((back_high[...], back_low[...]), halves(section))


def x_stage(plan, data, gains, tables):
    gain, shift, mirror = gains
    count = (gain.shape[0] + 1) // 2
    wide = count * LANES
    lane_block = pl.BlockSpec((plan.freq, wide), lambda i: (0, i))

    def whole(array):
        return pl.BlockSpec(array.shape, lambda i: (0,) * array.ndim)

    return pl.pallas_call(
        functools.partial(x_kernel, plan),
        grid=(plan.steps,),
        in_specs=[
            lane_block,
            pl.BlockSpec((gain.shape[0], 1, plan.spread, LANES), lambda i: (0, i, 0, 0)),
            whole(shift),
            whole(mirror),
            *[whole(t) for t in tables],
        ],
        out_specs=lane_block,
        out_shape=jax.ShapeDtypeStruct(data.shape, jnp.float32),
        scratch_shapes=[pltpu.VMEM((count, plan.spread, 2 * LANES), jnp.float32)],
        compiler_params=pltpu.CompilerParams(vmem_limit_bytes=50 * 2**20),
        cost_estimate=pl.CostEstimate(
            flops=24 * plan.freq * wide * plan.steps * 2 * plan.spread,
            bytes_accessed=12 * 2**20,
            transcendentals=0,
        ),
        name="x_stage",
    )(data, gain, shift, mirror, *tables)


def y_inverse_kernel(plan, place_ref, data_ref, high_ref, low_ref, turn_ref, out_ref, inner_ref, sum_ref):
    step = pl.program_id(0)
    value = dot_3((high_ref[0], low_ref[0]), halves(data_ref[...]))
    deep = 2 * LANES
    lane = lax.broadcasted_iota(jnp.int32, (1, LANES), 1)
    count = out_ref.shape[1]
    for comp in range(count):
        mixed = value[:deep, comp * LANES : (comp + 1) * LANES]
        for inner in range(1, plan.group):
            mixed = jnp.where(
                lane // plan.rows == inner,
                value[inner * deep : (inner + 1) * deep, comp * LANES : (comp + 1) * LANES],
                mixed,
            )
        inner_ref[comp, step] = mixed

    @pl.when(step == plan.steps - 1)
    def _():
        chunk = 8
        blocks = plan.block_y // LANES

        def one_comp(comp, carry):
            def one(index, carry):
                start = pl.multiple_of(index * chunk, chunk)
                items = [
                    (
                        inner_ref[comp, place, pl.ds(start, chunk), :],
                        inner_ref[comp, place, pl.ds(LANES + start, chunk), :],
                    )
                    for place in range(plan.steps)
                ]
                odd = jnp.where(lane < plan.rows, items[0][1], 0.0)
                period = 2 * plan.steps
                parts = fft(items + [None] * plan.steps, 1, list(range(period)))
                for block in range(plan.slots):
                    re, im = parts[block % period]
                    total = re * turn_ref[0, block : block + 1, :]
                    total = total - im * turn_ref[1, block : block + 1, :]
                    total = total + odd if block % 2 == 0 else total - odd
                    shift = LANES // 2
                    while shift >= plan.rows:
                        total = total + pltpu.roll(total, shift, 1)
                        shift //= 2
                    sum_ref[block, pl.ds(start, chunk), :] = total
                return carry

            lax.fori_loop(0, LANES // chunk, one, 0)
            for block in range(plan.slots):
                first = block % blocks * LANES
                target = lax.bitwise_xor(block // blocks, place_ref[0])
                out_ref[target, comp, :, first : first + LANES] = sum_ref[block].T[: plan.rows]
            return carry

        lax.fori_loop(0, count, one_comp, 0)


def y_inverse(plan, place, data, high, low):
    wide = data.shape[1] // plan.steps
    count = wide // LANES
    deep = plan.group * 2 * LANES
    matrix = pl.BlockSpec((1, deep, plan.freq), lambda i: (i, 0, 0))
    shape = (plan.n_ty, count, plan.rows, plan.block_y)
    inner = np.arange(LANES) // plan.rows
    angle = 2 * np.pi * np.outer(np.arange(plan.slots), inner) / plan.residues
    turn = jnp.asarray(np.stack([np.cos(angle), np.sin(angle)]), jnp.float32)
    return pl.pallas_call(
        functools.partial(y_inverse_kernel, plan),
        grid=(plan.steps,),
        in_specs=[
            pl.BlockSpec(memory_space=pltpu.SMEM),
            pl.BlockSpec((plan.freq, wide), lambda i: (0, i)),
            matrix,
            matrix,
            pl.BlockSpec(turn.shape, lambda i: (0, 0, 0)),
        ],
        out_specs=pl.BlockSpec(shape, lambda i: (0, 0, 0, 0)),
        out_shape=jax.ShapeDtypeStruct(shape, jnp.float32),
        scratch_shapes=[
            pltpu.VMEM((count, plan.steps, 2 * LANES, LANES), jnp.float32),
            pltpu.VMEM((plan.slots, LANES, LANES), jnp.float32),
        ],
        compiler_params=pltpu.CompilerParams(vmem_limit_bytes=50 * 2**20),
        cost_estimate=pl.CostEstimate(
            flops=6 * plan.freq * wide * plan.steps * deep,
            bytes_accessed=10 * 2**20,
            transcendentals=0,
        ),
        name="y_inverse",
    )(place, data, high, low, turn)


def kernel_gains(plan, kernel, diagonal):
    n, near, slots = plan.devices, plan.near, plan.slots
    me = lax.axis_index(AXES)
    scale = 2.0 / (plan.len_x * plan.len_y)
    kx = np.arange(plan.len_x)
    wave_x = jnp.asarray(2 * STIFFNESS * np.cos(2 * np.pi * kx / plan.len_x), jnp.float32)
    count = kernel.shape[0]
    diagonal = jnp.asarray(diagonal, jnp.float32)

    nyquist = lax.ppermute(kernel[:, 0, :], AXES, [(n // 2, 0)])
    split = kernel.reshape(count, near, plan.residues, plan.len_x)
    first = jnp.where(me < n // 2, split[:, :, :1], split[:, :, slots : slots + 1])
    chosen = jnp.concatenate([first, split[:, :, 1:slots]], axis=2)
    slot = lax.broadcasted_iota(jnp.int32, (near, slots), 1)
    slot = jnp.where((slot == 0) & (me >= n // 2), slots, slot)
    ky = (me * near + lax.broadcasted_iota(jnp.int32, (near, slots), 0)) * plan.residues + slot
    wave_y = 2 * STIFFNESS * jnp.cos(ky.astype(jnp.float32) * (2 * math.pi / plan.len_y))
    wave = wave_x[None, None, :] + wave_y[:, :, None]
    gain = (diagonal[:, None, None, None] * wave[None] - chosen) * scale

    def arrange(array, count_near, count_slots):
        group = min(plan.group, count_slots)
        shaped = array.reshape(count, count_near, count_slots // group, group, plan.rows, 2 * n)
        moved = shaped.transpose(0, 2, 5, 1, 3, 4)
        return moved.reshape(count, count_slots // group, 2 * n * count_near, group * plan.rows)

    zero_row = (diagonal[:, None] * (wave_x + 2 * STIFFNESS)[None] - kernel[:, 0, :]) * scale
    last_row = (diagonal[:, None] * (wave_x - 2 * STIFFNESS)[None] - nyquist) * scale
    shift = jnp.where(me == 0, 0.25 * (zero_row + last_row) - zero_row, 0.0)
    mirror = jnp.where(me == 0, 0.25 * (zero_row - last_row), 0.0)

    def place(row):
        small = row.reshape(count, plan.rows, 2 * n).transpose(0, 2, 1)[:, :, None, :]
        small = jnp.pad(small, ((0, 0), (0, 0), (0, near - 1), (0, LANES - plan.rows)))
        return small.reshape(count, plan.spread, LANES)

    arrays = (arrange(gain, near, slots), place(shift), place(mirror))
    return arrays


def cross(left, right):
    return jnp.stack(
        [
            left[1] * right[2] - left[2] * right[1],
            left[2] * right[0] - left[0] * right[2],
            left[0] * right[1] - left[1] * right[0],
        ]
    )


def swap(values, axis, offset):
    size = lax.axis_size(axis)
    return lax.ppermute(values, axis, [(i, i ^ offset) for i in range(size)])


def exchange(values, axes):
    return lax.all_to_all(values, axes, split_axis=0, concat_axis=0, tiled=True)


def body(mag, occupancy, kernel_spectrum):
    plan = Plan(mag.shape, lax.axis_size("tx"), lax.axis_size("ty"))
    occ = occupancy.astype(jnp.float32)
    start = mag * occ[None]
    matrix = plan.y_matrices()
    rounded = lax.reduce_precision(matrix, 8, 7)
    high, low = rounded.astype(jnp.bfloat16), (matrix - rounded).astype(jnp.bfloat16)
    high_back, low_back = jnp.swapaxes(high, 1, 2), jnp.swapaxes(low, 1, 2)
    one = plan.x_first()
    tables = (
        *np_halves(one),
        *np_halves(one.T),
        *np_halves(plan.x_second()),
        jnp.asarray(plan.x_turn()),
    )
    gain_b = kernel_gains(plan, kernel_spectrum[2:3], (1.0,))
    paired = jnp.concatenate([kernel_spectrum[:2], kernel_spectrum[3:]])
    gain_a = kernel_gains(plan, paired, (1.0, 1.0, 0.0))

    def sent(array):
        return array.reshape(plan.devices, 2 * plan.near, array.shape[1])

    def flat(array):
        return array.reshape(plan.freq, array.shape[2])

    here = lax.axis_index("ty")
    place = here.reshape(1)

    def start_row(offset):
        return (here ^ offset) * plan.rows

    def gather_rows(field):
        size = (field.shape[0], plan.rows, plan.block_y)
        pieces = []
        for offset in range(plan.n_ty):
            piece = lax.dynamic_slice(field, (0, start_row(offset), 0), size)
            pieces.append(swap(piece, "ty", offset) if offset else piece)
        return jnp.stack(pieces)

    def return_rows(spatial):
        count = spatial.shape[1]
        field = jnp.zeros((count, plan.block_x, plan.block_y), jnp.float32)
        for offset in range(plan.n_ty):
            piece = swap(spatial[offset], "ty", offset) if offset else spatial[0]
            field = lax.dynamic_update_slice(field, piece, (0, start_row(offset), 0))
        return field

    def effective(field):
        rows_a = gather_rows(field[:2])
        rows_b = gather_rows(field[2:])
        spectra_a = sent(y_forward(plan, place, rows_a, high, low))
        columns_a = exchange(spectra_a, AXES)
        spectra_b = sent(y_forward(plan, place, rows_b, high, low))
        columns_a, spectra_b = lax.optimization_barrier((columns_a, spectra_b))
        columns_b = exchange(spectra_b, AXES)
        product_a = sent(x_stage(plan, flat(columns_a), gain_a, tables))
        product_a, columns_b = lax.optimization_barrier((product_a, columns_b))
        returned_a = exchange(product_a, AXES)
        product_b = sent(x_stage(plan, flat(columns_b), gain_b, tables))
        returned_a, product_b = lax.optimization_barrier((returned_a, product_b))
        returned_b = exchange(product_b, AXES)
        spatial_a = y_inverse(plan, place, flat(returned_a), high_back, low_back)
        field_a = return_rows(spatial_a)
        spatial_b = y_inverse(plan, place, flat(returned_b), high_back, low_back)
        field_b = return_rows(spatial_b)
        return jnp.concatenate([field_a, field_b])

    def rate(field):
        torque = cross(field, effective(field))
        return -(torque + DAMPING * cross(field, torque)) / (1.0 + DAMPING * DAMPING)

    def normal(vector):
        return vector / jnp.sqrt(jnp.sum(vector * vector, axis=0) + 1.0 - occ)[None]

    first = rate(start)
    middle = normal(start + TIME_STEP * first)
    second = rate(middle)
    second = second - jnp.sum(second * start, axis=0)[None] * start
    mean_rate = 0.5 * (first + second)
    mag_next = normal(start + TIME_STEP * mean_rate)
    return (mag_next, mean_rate)


def solution(mesh):
    return jax.shard_map(
        body,
        mesh=mesh,
        in_specs=(P(None, "tx", "ty"), P("tx", "ty"), P(None, ("tx", "ty"), None)),
        out_specs=(P(None, "tx", "ty"), P(None, "tx", "ty")),
        check_vma=False,
    )
```

```python
import functools
import math

import jax
import jax.numpy as jnp
import numpy as np
from jax import lax
from jax.experimental import pallas as pl
from jax.experimental.pallas import tpu as pltpu
from jax.sharding import PartitionSpec as P

DAMPING = 0.3
STIFFNESS = 0.25
TIME_STEP = 0.25
LANES = 128
AXES = ("tx", "ty")


def halves(values):
    high = values.astype(jnp.bfloat16)
    low = (values - high.astype(jnp.float32)).astype(jnp.bfloat16)
    return high, low


def np_halves(values):
    values = np.asarray(values, np.float64)
    high = values.astype(np.float32).astype(jnp.bfloat16)
    low = (values - high.astype(np.float64)).astype(np.float32).astype(jnp.bfloat16)
    return jnp.asarray(high), jnp.asarray(low)


def dot(left, right, dims):
    return lax.dot_general(left, right, (dims, ((), ())), preferred_element_type=jnp.float32)


def dot_3(left, right, dims=((1,), (0,))):
    return (
        dot(left[0], right[0], dims) + dot(left[1], right[0], dims) + dot(left[0], right[1], dims)
    )


NT = ((1,), (1,))


def c_add(a, b):
    if a is None:
        return b
    if b is None:
        return a
    re = a[0] + b[0]
    if a[1] is None or b[1] is None:
        return (re, b[1] if a[1] is None else a[1])
    return (re, a[1] + b[1])


def c_sub(a, b):
    if b is None:
        return a
    re = a[0] - b[0]
    if b[1] is None:
        return (re, a[1])
    return (re, -b[1] if a[1] is None else a[1] - b[1])


def c_turn(a, num, den, sign):
    num %= den
    if a is None or num == 0:
        return a
    re, im = a
    if 4 * num == den:
        return (None, sign * re) if im is None else (-sign * im, sign * re)
    cos, sin = math.cos(2 * math.pi * num / den), sign * math.sin(2 * math.pi * num / den)
    if im is None:
        return (re * cos, re * sin)
    return (re * cos - im * sin, re * sin + im * cos)


def fix(a):
    if a is not None and a[0] is None:
        return (jnp.zeros_like(a[1]), a[1])
    return a


def fft(items, sign, wanted):
    size = len(items)
    if size == 1:
        return {0: items[0]}
    half = size // 2
    result = {}
    even = sorted({k // 2 for k in wanted if k % 2 == 0})
    odd = sorted({k // 2 for k in wanted if k % 2 == 1})
    if even:
        sub = fft([c_add(items[i], items[i + half]) for i in range(half)], sign, even)
        result.update({2 * k: v for k, v in sub.items()})
    if odd:
        parts = [
            fix(c_turn(c_sub(items[i], items[i + half]), i, size, sign)) for i in range(half)
        ]
        result.update({2 * k + 1: v for k, v in fft(parts, sign, odd).items()})
    return result


class Plan:
    def __init__(self, mag_shape, n_tx, n_ty):
        self.n_ty = n_ty
        self.devices = n = n_tx * n_ty
        self.block_x, self.block_y = mag_shape[1:]
        self.rows = self.block_x // n_ty
        self.len_x, self.len_y = 2 * self.block_x * n_tx, 2 * self.block_y * n_ty
        self.slots = self.len_y // 2 // LANES
        self.residues = 2 * self.slots
        self.near = self.len_y // n // self.residues
        self.group = LANES // self.rows
        self.steps = self.slots // self.group
        self.freq = n * 2 * self.near
        self.spread = 2 * n * self.near
        self.split = 4 * n == LANES and self.group == 2
        lane = np.arange(LANES)
        self.lane_slot, self.lane_kappa = lane // self.rows, lane % self.rows
        if self.split:
            fine = LANES // 4
            self.lane_slot = lane // fine % 2
            self.lane_kappa = 2 * (lane % fine) + lane // (2 * fine)

    def y_tables(self):
        k1 = np.arange(LANES)
        spot = np.arange(LANES)
        angle = 2 * np.pi * np.outer(k1, spot) / LANES
        cos, sin = np.cos(angle), np.sin(angle)

        def rows(re_re, re_im, im_re, im_im):
            full = np.stack(
                [np.concatenate([re_re, re_im], 1), np.concatenate([im_re, im_im], 1)]
            )
            full = full.reshape(2, self.devices, self.near, 2 * LANES)
            return full.transpose(1, 0, 2, 3).reshape(self.freq, 2 * LANES)

        plain = rows(cos, sin, -sin, cos)
        mixed = rows(-sin, cos, -cos, -sin)
        slot = np.arange(self.slots)
        turn = 2 * np.pi * np.outer(slot, spot) / self.len_y
        turn_cos = np.tile(np.cos(turn), 2).reshape(self.steps, 1, self.group * 2 * LANES)
        turn_sin = np.tile(np.sin(turn), 2).reshape(self.steps, 1, self.group * 2 * LANES)
        late = 2 * np.pi * np.outer(k1 + 0.5, spot) / LANES
        low = (k1 < LANES // 2)[:, None]
        zero = np.zeros_like(cos)
        im_first = np.where(low, -sin, 0)
        im_first[0] = np.cos(np.pi * spot)
        first = rows(
            np.where(low, cos, zero),
            np.where(low, zero, np.cos(late)),
            im_first,
            np.where(low, zero, -np.sin(late)),
        )
        return plain, mixed, turn_cos, turn_sin, first

    def y_matrices(self):
        plain, mixed, turn_cos, turn_sin, first = (
            jnp.asarray(t, jnp.float32) for t in self.y_tables()
        )
        plain = jnp.concatenate([plain] * self.group, axis=1)[None]
        mixed = jnp.concatenate([mixed] * self.group, axis=1)[None]
        full = plain * turn_cos + mixed * turn_sin
        first = jnp.pad(first, ((0, 0), (0, (self.group - 1) * 2 * LANES)))[None]
        shape = (self.steps, 1, self.group * 2 * LANES)
        at_first = (lax.broadcasted_iota(jnp.int32, shape, 0) == 0) & (
            lax.broadcasted_iota(jnp.int32, shape, 2) < 2 * LANES
        )
        return jnp.where(at_first, first, full)

    def x_first(self):
        n = self.devices
        angle = 2 * np.pi * np.outer(np.arange(2 * n), np.arange(n)) / (2 * n)
        cos, sin = np.cos(angle), np.sin(angle)
        table = np.stack([np.stack([cos, sin], -1), np.stack([-sin, cos], -1)])
        full = np.einsum("orsi,fg->ofrsig", table, np.eye(self.near))
        return full.reshape(2 * self.spread, self.freq)

    def x_turn(self):
        angle = -2 * np.pi * np.outer(np.arange(2 * self.devices), np.arange(self.rows))
        angle = np.tile(angle / self.len_x, (self.near, self.group))
        return np.stack([np.cos(angle), np.sin(angle)]).astype(np.float32)

    def x_second(self):
        span = np.arange(self.rows)
        angle = 2 * np.pi * np.outer(span, span) / self.rows
        cos, sin = np.cos(angle), np.sin(angle)
        table = np.stack([np.stack([cos, -sin], 1), np.stack([sin, cos], 1)])
        full = np.einsum("ixok,qp->iqxopk", table, np.eye(self.group))
        full = full[:, :, :, :, self.lane_slot, self.lane_kappa]
        return full.reshape(2 * LANES, 2 * LANES)


def y_forward_kernel(plan, place_ref, rows_ref, high_ref, low_ref, out_ref, z_high, z_low):
    step = pl.program_id(0)
    chunk = 16
    per = plan.rows // chunk
    blocks = plan.block_y // LANES

    @pl.when(step == 0)
    def _():
        if plan.group > 1:
            z_high[...] = jnp.zeros_like(z_high)
            z_low[...] = jnp.zeros_like(z_low)

        def one(index, carry):
            comp = index // per
            start = pl.multiple_of((index % per) * chunk, chunk)
            items = []
            for block in range(plan.slots):
                lane = block % blocks * LANES
                items.append(
                    (
                        rows_ref[
                            lax.bitwise_xor(block // blocks, place_ref[0]),
                            comp,
                            pl.ds(start, chunk),
                            lane : lane + LANES,
                        ],
                        None,
                    )
                )
            items += [None] * plan.slots
            parts = fft(items, -1, list(range(plan.slots + 1)))
            for slot in range(plan.slots):
                pair = (parts[0][0], parts[plan.slots][0]) if slot == 0 else parts[slot]
                place, inner = slot // plan.group, slot % plan.group
                row = pl.multiple_of(comp * LANES + inner * plan.rows + start, chunk)
                for half in range(2):
                    lane = inner * 2 * LANES + half * LANES
                    high, low = halves(pair[half])
                    z_high[place, pl.ds(row, chunk), lane : lane + LANES] = high
                    z_low[place, pl.ds(row, chunk), lane : lane + LANES] = low
            return carry

        lax.fori_loop(0, rows_ref.shape[1] * per, one, 0)

    left = (high_ref[0], low_ref[0])
    out_ref[...] = dot_3(left, (z_high[step], z_low[step]), NT)


def y_forward(plan, place, rows, high, low):
    wide = rows.shape[1] * LANES
    deep = plan.group * 2 * LANES
    matrix = pl.BlockSpec((1, plan.freq, deep), lambda i: (i, 0, 0))
    return pl.pallas_call(
        functools.partial(y_forward_kernel, plan),
        grid=(plan.steps,),
        in_specs=[
            pl.BlockSpec(memory_space=pltpu.SMEM),
            pl.BlockSpec(rows.shape, lambda i: (0, 0, 0, 0)),
            matrix,
            matrix,
        ],
        out_specs=pl.BlockSpec((plan.freq, wide), lambda i: (0, i)),
        out_shape=jax.ShapeDtypeStruct((plan.freq, wide * plan.steps), jnp.float32),
        scratch_shapes=[
            pltpu.VMEM((plan.steps, wide, deep), jnp.bfloat16),
            pltpu.VMEM((plan.steps, wide, deep), jnp.bfloat16),
        ],
        compiler_params=pltpu.CompilerParams(vmem_limit_bytes=50 * 2**20),
        cost_estimate=pl.CostEstimate(
            flops=6 * plan.freq * wide * plan.steps * deep,
            bytes_accessed=10 * 2**20,
            transcendentals=0,
        ),
        name="y_forward",
    )(place, rows, high, low)


def x_kernel(
    plan,
    data_ref,
    gain_ref,
    shift_ref,
    mirror_ref,
    one_high,
    one_low,
    back_high,
    back_low,
    two_high,
    two_low,
    turn_ref,
    out_ref,
    field_ref,
):
    one = (one_high[...], one_low[...])
    two = (two_high[...], two_low[...])
    turn_re, turn_im = turn_ref[0], turn_ref[1]
    size = plan.spread
    count = field_ref.shape[0]

    def cut(comp):
        return slice(comp * LANES, (comp + 1) * LANES)

    def spectrum(data):
        section = dot_3(one, halves(data))
        result = []
        for comp in range(count):
            re, im = section[:size, cut(comp)], section[size:, cut(comp)]
            turned = jnp.concatenate(
                [re * turn_re - im * turn_im, re * turn_im + im * turn_re], axis=1
            )
            result.append(dot_3(halves(turned), two))
        return result

    def apply(gain, parts):
        wide = [jnp.concatenate([gain(i)] * 2, axis=1) for i in range(2 * count - 1)]
        if count == 1:
            return [wide[0] * parts[0]]
        return [
            wide[0] * parts[0] + wide[2] * parts[1],
            wide[2] * parts[0] + wide[1] * parts[1],
        ]

    data = data_ref[...]
    parts = spectrum(data)
    for comp, value in enumerate(apply(lambda i: gain_ref[i, 0], parts)):
        field_ref[comp] = value

    @pl.when(pl.program_id(0) == 0)
    def _():
        row = lax.broadcasted_iota(jnp.int32, (plan.freq, 1), 0)
        sign = jnp.where(row // plan.near % 2 == 0, 1.0, -1.0)
        other = spectrum(data * sign)
        added = apply(lambda i: shift_ref[i], parts)
        flipped = apply(lambda i: mirror_ref[i], other)
        for comp in range(count):
            field_ref[comp] += added[comp] + flipped[comp]

    re_list, im_list = [], []
    for comp in range(count):
        value = dot_3(halves(field_ref[comp]), two, NT)
        re, im = value[:, :LANES], value[:, LANES:]
        re_list.append(re * turn_re + im * turn_im)
        im_list.append(im * turn_re - re * turn_im)
    section = jnp.concatenate(
        [jnp.concatenate(re_list, axis=1), jnp.concatenate(im_list, axis=1)], axis=0
    )
    out_ref[...] = dot_3((back_high[...], back_low[...]), halves(section))


def x_stage(plan, data, gains, group, tables):
    gain, shift, mirror = gains
    size, index = group
    count = (size + 1) // 2
    wide = count * LANES
    lane_block = pl.BlockSpec((plan.freq, wide), lambda i: (0, i))

    def whole(array):
        return pl.BlockSpec(array.shape, lambda i: (0,) * array.ndim)

    return pl.pallas_call(
        functools.partial(x_kernel, plan),
        grid=(plan.steps,),
        in_specs=[
            lane_block,
            pl.BlockSpec((size, 1, plan.spread, LANES), lambda i: (index, i, 0, 0)),
            pl.BlockSpec((size, plan.spread, LANES), lambda i: (index, 0, 0)),
            pl.BlockSpec((size, plan.spread, LANES), lambda i: (index, 0, 0)),
            *[whole(t) for t in tables],
        ],
        out_specs=lane_block,
        out_shape=jax.ShapeDtypeStruct(data.shape, jnp.float32),
        scratch_shapes=[pltpu.VMEM((count, plan.spread, 2 * LANES), jnp.float32)],
        compiler_params=pltpu.CompilerParams(vmem_limit_bytes=50 * 2**20),
        cost_estimate=pl.CostEstimate(
            flops=24 * plan.freq * wide * plan.steps * 2 * plan.spread,
            bytes_accessed=12 * 2**20,
            transcendentals=0,
        ),
        name="x_stage",
    )(data, gain, shift, mirror, *tables)


def y_inverse_kernel(plan, place_ref, data_ref, high_ref, low_ref, turn_ref, out_ref, inner_ref, sum_ref):
    step = pl.program_id(0)
    value = dot_3((high_ref[0], low_ref[0]), halves(data_ref[...]))
    deep = 2 * LANES
    lane = lax.broadcasted_iota(jnp.int32, (1, LANES), 1)
    count = out_ref.shape[1]
    for comp in range(count):
        mixed = value[:deep, comp * LANES : (comp + 1) * LANES]
        for inner in range(1, plan.group):
            mixed = jnp.where(
                lane // plan.rows == inner,
                value[inner * deep : (inner + 1) * deep, comp * LANES : (comp + 1) * LANES],
                mixed,
            )
        inner_ref[comp, step] = mixed

    @pl.when(step == plan.steps - 1)
    def _():
        chunk = 8
        blocks = plan.block_y // LANES

        def one_comp(comp, carry):
            def one(index, carry):
                start = pl.multiple_of(index * chunk, chunk)
                items = [
                    (
                        inner_ref[comp, place, pl.ds(start, chunk), :],
                        inner_ref[comp, place, pl.ds(LANES + start, chunk), :],
                    )
                    for place in range(plan.steps)
                ]
                odd = jnp.where(lane < plan.rows, items[0][1], 0.0)
                period = 2 * plan.steps
                parts = fft(items + [None] * plan.steps, 1, list(range(period)))
                for block in range(plan.slots):
                    re, im = parts[block % period]
                    total = re * turn_ref[0, block : block + 1, :]
                    total = total - im * turn_ref[1, block : block + 1, :]
                    total = total + odd if block % 2 == 0 else total - odd
                    shift = LANES // 2
                    while shift >= plan.rows:
                        total = total + pltpu.roll(total, shift, 1)
                        shift //= 2
                    sum_ref[block, pl.ds(start, chunk), :] = total
                return carry

            lax.fori_loop(0, LANES // chunk, one, 0)
            for block in range(plan.slots):
                first = block % blocks * LANES
                target = lax.bitwise_xor(block // blocks, place_ref[0])
                out_ref[target, comp, :, first : first + LANES] = sum_ref[block].T[: plan.rows]
            return carry

        lax.fori_loop(0, count, one_comp, 0)


def y_inverse(plan, place, data, high, low):
    wide = data.shape[1] // plan.steps
    count = wide // LANES
    deep = plan.group * 2 * LANES
    matrix = pl.BlockSpec((1, deep, plan.freq), lambda i: (i, 0, 0))
    shape = (plan.n_ty, count, plan.rows, plan.block_y)
    inner = np.arange(LANES) // plan.rows
    angle = 2 * np.pi * np.outer(np.arange(plan.slots), inner) / plan.residues
    turn = jnp.asarray(np.stack([np.cos(angle), np.sin(angle)]), jnp.float32)
    return pl.pallas_call(
        functools.partial(y_inverse_kernel, plan),
        grid=(plan.steps,),
        in_specs=[
            pl.BlockSpec(memory_space=pltpu.SMEM),
            pl.BlockSpec((plan.freq, wide), lambda i: (0, i)),
            matrix,
            matrix,
            pl.BlockSpec(turn.shape, lambda i: (0, 0, 0)),
        ],
        out_specs=pl.BlockSpec(shape, lambda i: (0, 0, 0, 0)),
        out_shape=jax.ShapeDtypeStruct(shape, jnp.float32),
        scratch_shapes=[
            pltpu.VMEM((count, plan.steps, 2 * LANES, LANES), jnp.float32),
            pltpu.VMEM((plan.slots, LANES, LANES), jnp.float32),
        ],
        compiler_params=pltpu.CompilerParams(vmem_limit_bytes=50 * 2**20),
        cost_estimate=pl.CostEstimate(
            flops=6 * plan.freq * wide * plan.steps * deep,
            bytes_accessed=10 * 2**20,
            transcendentals=0,
        ),
        name="y_inverse",
    )(place, data, high, low, turn)


ORDER = (0, 1, 3, 2)


def gain_kernel(plan, scale, late_ref, kernel_ref, wave_x_ref, wave_y_ref, out_ref, sort_ref):
    slots = plan.slots
    blocks = plan.len_x // LANES
    row = lax.broadcasted_iota(jnp.int32, (slots, 1), 0)
    lane = lax.broadcasted_iota(jnp.int32, (1, LANES), 1)
    swapped = (row == 0) & (late_ref[0] == 1)
    for block in range(blocks):
        span = slice(block * LANES, (block + 1) * LANES)
        value = kernel_ref[0, :slots, span]
        value = jnp.where(swapped, kernel_ref[0, slots : slots + 1, span], value)
        sort_ref[pl.ds(block, slots, stride=blocks), :] = value
    diagonal = jnp.where(pl.program_id(0) == 2, 0.0, scale)
    half = LANES // 2
    for pair in range(plan.steps // 2):
        turned = sort_ref[pair * LANES : (pair + 1) * LANES, :].T
        low, high = turned[:half], turned[half:]
        parts = (
            jnp.where(lane < half, low, pltpu.roll(high, half, 1)),
            jnp.where(lane < half, pltpu.roll(low, half, 1), high),
        )
        for i, part in enumerate(parts):
            step = 2 * pair + i
            wave = wave_x_ref[...] + wave_y_ref[0, step : step + 1, :]
            out_ref[0, step] = diagonal * wave - scale * part


def kernel_gains(plan, kernel):
    n, near, slots = plan.devices, plan.near, plan.slots
    me = lax.axis_index(AXES)
    scale = 2.0 / (plan.len_x * plan.len_y)
    r = np.arange(2 * n)
    kx = 2 * n * plan.lane_kappa[None] + r[:, None]
    wave_x = jnp.asarray(2 * STIFFNESS * np.cos(2 * np.pi * kx / plan.len_x), jnp.float32)
    late = me >= n // 2
    slot = lax.broadcasted_iota(jnp.int32, (near, slots), 1)
    slot = jnp.where((slot == 0) & late, slots, slot)
    ky = (me * near + lax.broadcasted_iota(jnp.int32, (near, slots), 0)) * plan.residues + slot
    wave_y = 2 * STIFFNESS * jnp.cos(ky.astype(jnp.float32) * (2 * math.pi / plan.len_y))
    wave_y = wave_y.reshape(near, plan.steps, plan.group)
    wave_y = sum(
        wave_y[:, :, i : i + 1] * jnp.asarray(plan.lane_slot == i, jnp.float32)
        for i in range(plan.group)
    )
    if plan.split:
        out_shape = (4, plan.steps, plan.spread, LANES)
        gain = pl.pallas_call(
            functools.partial(gain_kernel, plan, scale),
            grid=(4, near),
            in_specs=[
                pl.BlockSpec(memory_space=pltpu.SMEM),
                pl.BlockSpec(
                    (1, plan.residues, plan.len_x),
                    lambda c, f: (jnp.where(c < 2, c, 5 - c), f, 0),
                ),
                pl.BlockSpec(wave_x.shape, lambda c, f: (0, 0)),
                pl.BlockSpec((1, plan.steps, LANES), lambda c, f: (f, 0, 0)),
            ],
            out_specs=pl.BlockSpec((1, plan.steps, 2 * n, LANES), lambda c, f: (c, 0, f, 0)),
            out_shape=jax.ShapeDtypeStruct(out_shape, jnp.float32),
            scratch_shapes=[pltpu.VMEM((slots * plan.len_x // LANES, LANES), jnp.float32)],
            compiler_params=pltpu.CompilerParams(vmem_limit_bytes=16 * 2**20),
            cost_estimate=pl.CostEstimate(
                flops=2**30, bytes_accessed=12 * 2**20, transcendentals=0
            ),
            name="gain",
        )(late.astype(jnp.int32).reshape(1), kernel, wave_x, wave_y)
    else:
        kernel_4 = kernel.reshape(4, near, plan.residues, plan.len_x)
        first = jnp.where(late, kernel_4[:, :, slots : slots + 1], kernel_4[:, :, :1])
        chosen = jnp.concatenate([first, kernel_4[:, :, 1:slots]], axis=2)
        shaped = chosen.reshape(4, near, plan.steps, plan.group, plan.rows, 2 * n)
        moved = shaped.transpose(0, 2, 1, 5, 3, 4).reshape(4, plan.steps, near, 2 * n, LANES)
        moved = jnp.stack([moved[i] for i in ORDER])
        wave = wave_x + wave_y.transpose(1, 0, 2)[:, :, None]
        gain = jnp.concatenate([wave[None] - moved[:2], -moved[2:3], wave[None] - moved[3:]])
        gain = (scale * gain).reshape(4, plan.steps, plan.spread, LANES)

    nyquist = lax.ppermute(kernel[:, 0, :], AXES, [(n // 2, 0)])

    def arrange(row, wave_y):
        row = jnp.stack([row[i] for i in ORDER])
        if plan.split:
            small = row.reshape(4, plan.rows // 2, 2, 2 * n).transpose(0, 3, 2, 1)
        else:
            small = row.reshape(4, plan.rows, 1, 2 * n).transpose(0, 3, 2, 1)
        small = jnp.pad(small[:, :, :, None], ((0, 0),) * 3 + ((0, plan.group - 1), (0, 0)))
        small = small.reshape(4, 2 * n, LANES)
        diagonal = jnp.asarray([1.0, 1.0, 0.0, 1.0], jnp.float32)[:, None, None]
        return (diagonal * (wave_x + wave_y) - small) * scale

    zero_row = arrange(kernel[:, 0, :], 2 * STIFFNESS)
    last_row = arrange(nyquist, -2 * STIFFNESS)
    used = jnp.asarray(plan.lane_slot == 0) & (me == 0)

    def place(rows):
        rows = jnp.where(used, rows, 0.0)[:, None]
        rows = jnp.pad(rows, ((0, 0), (0, near - 1), (0, 0), (0, 0)))
        return rows.reshape(4, plan.spread, LANES)

    shift = place(0.25 * (zero_row + last_row) - zero_row)
    return gain, shift, place(0.25 * (zero_row - last_row))


def cross(left, right):
    return [
        left[1] * right[2] - left[2] * right[1],
        left[2] * right[0] - left[0] * right[2],
        left[0] * right[1] - left[1] * right[0],
    ]


def inner(left, right):
    return left[0] * right[0] + left[1] * right[1] + left[2] * right[2]


def rate(field, effective):
    torque = cross(field, effective)
    again = cross(field, torque)
    return [-(t + DAMPING * a) / (1.0 + DAMPING * DAMPING) for t, a in zip(torque, again)]


def normal(vector, occ):
    size = jnp.sqrt(inner(vector, vector) + 1.0 - occ)
    return [v / size for v in vector]


def swap(values, axis, offset):
    size = lax.axis_size(axis)
    return lax.ppermute(values, axis, [(i, i ^ offset) for i in range(size)])


def exchange(values, axes):
    return lax.all_to_all(values, axes, split_axis=0, concat_axis=0, tiled=True)


def body(mag, occupancy, kernel_spectrum):
    plan = Plan(mag.shape, lax.axis_size("tx"), lax.axis_size("ty"))
    occ = occupancy.astype(jnp.float32)
    start = mag * occ[None]
    matrix = plan.y_matrices()
    rounded = lax.reduce_precision(matrix, 8, 7)
    high, low = rounded.astype(jnp.bfloat16), (matrix - rounded).astype(jnp.bfloat16)
    high_back, low_back = jnp.swapaxes(high, 1, 2), jnp.swapaxes(low, 1, 2)
    one = plan.x_first()
    tables = (
        *np_halves(one),
        *np_halves(one.T),
        *np_halves(plan.x_second()),
        jnp.asarray(plan.x_turn()),
    )
    gains = kernel_gains(plan, kernel_spectrum)

    def sent(array):
        return array.reshape(plan.devices, 2 * plan.near, array.shape[1])

    def flat(array):
        return array.reshape(plan.freq, array.shape[2])

    here = lax.axis_index("ty")
    place = here.reshape(1)

    def start_row(offset):
        return (here ^ offset) * plan.rows

    def gather_rows(field):
        size = (field.shape[0], plan.rows, plan.block_y)
        pieces = []
        for offset in range(plan.n_ty):
            piece = lax.dynamic_slice(field, (0, start_row(offset), 0), size)
            pieces.append(swap(piece, "ty", offset) if offset else piece)
        return jnp.stack(pieces)

    def return_rows(spatial):
        count = spatial.shape[1]
        field = jnp.zeros((count, plan.block_x, plan.block_y), jnp.float32)
        for offset in range(plan.n_ty):
            piece = swap(spatial[offset], "ty", offset) if offset else spatial[0]
            field = lax.dynamic_update_slice(field, piece, (0, start_row(offset), 0))
        return field

    def effective(rows_a, rows_b):
        spectra_a = sent(y_forward(plan, place, rows_a, high, low))
        columns_a = exchange(spectra_a, AXES)
        spectra_b = sent(y_forward(plan, place, rows_b, high, low))
        columns_a, spectra_b = lax.optimization_barrier((columns_a, spectra_b))
        columns_b = exchange(spectra_b, AXES)
        product_a = sent(x_stage(plan, flat(columns_a), gains, (1, 3), tables))
        product_a, columns_b = lax.optimization_barrier((product_a, columns_b))
        returned_a = exchange(product_a, AXES)
        product_b = sent(x_stage(plan, flat(columns_b), gains, (3, 0), tables))
        returned_a, product_b = lax.optimization_barrier((returned_a, product_b))
        returned_b = exchange(product_b, AXES)
        field_a = y_inverse(plan, place, flat(returned_a), high_back, low_back)
        field_b = y_inverse(plan, place, flat(returned_b), high_back, low_back)
        return [field_b[:, 0], field_b[:, 1], field_a[:, 0]]

    rows_a = gather_rows(start[2:])
    rows_b = gather_rows(start[:2])
    field = effective(rows_a, rows_b)
    begin = [rows_b[:, 0], rows_b[:, 1], rows_a[:, 0]]
    held = jnp.where(inner(begin, begin) > 0.25, 1.0, 0.0)
    first = rate(begin, field)
    middle = normal([b + TIME_STEP * f for b, f in zip(begin, first)], held)
    field = effective(middle[2][:, None], jnp.stack(middle[:2], axis=1))
    second = rate(middle, field)
    along = inner(second, begin)
    mean = [0.5 * (f + (s - along * b)) for f, s, b in zip(first, second, begin)]
    mean_rate = return_rows(jnp.stack(mean, axis=1))
    moved = start + TIME_STEP * mean_rate
    return (jnp.stack(normal([moved[0], moved[1], moved[2]], occ)), mean_rate)


def solution(mesh):
    return jax.shard_map(
        body,
        mesh=mesh,
        in_specs=(P(None, "tx", "ty"), P("tx", "ty"), P(None, ("tx", "ty"), None)),
        out_specs=(P(None, "tx", "ty"), P(None, "tx", "ty")),
        check_vma=False,
    )
```

```python
import functools
import math

import jax
import jax.numpy as jnp
import numpy as np
from jax import lax
from jax.experimental import pallas as pl
from jax.experimental.pallas import tpu as pltpu
from jax.sharding import PartitionSpec as P

DAMPING = 0.3
STIFFNESS = 0.25
TIME_STEP = 0.25
LANES = 128
AXES = ("tx", "ty")


def halves(values):
    high = values.astype(jnp.bfloat16)
    low = (values - high.astype(jnp.float32)).astype(jnp.bfloat16)
    return high, low


def np_halves(values):
    values = np.asarray(values, np.float64)
    high = values.astype(np.float32).astype(jnp.bfloat16)
    low = (values - high.astype(np.float64)).astype(np.float32).astype(jnp.bfloat16)
    return jnp.asarray(high), jnp.asarray(low)


def dot(left, right, dims):
    return lax.dot_general(left, right, (dims, ((), ())), preferred_element_type=jnp.float32)


def dot_3(left, right, dims=((1,), (0,))):
    return (
        dot(left[0], right[0], dims) + dot(left[1], right[0], dims) + dot(left[0], right[1], dims)
    )


NT = ((1,), (1,))


def c_add(a, b):
    if a is None:
        return b
    if b is None:
        return a
    re = a[0] + b[0]
    if a[1] is None or b[1] is None:
        return (re, b[1] if a[1] is None else a[1])
    return (re, a[1] + b[1])


def c_sub(a, b):
    if b is None:
        return a
    re = a[0] - b[0]
    if b[1] is None:
        return (re, a[1])
    return (re, -b[1] if a[1] is None else a[1] - b[1])


def c_turn(a, num, den, sign):
    num %= den
    if a is None or num == 0:
        return a
    re, im = a
    if 4 * num == den:
        return (None, sign * re) if im is None else (-sign * im, sign * re)
    cos, sin = math.cos(2 * math.pi * num / den), sign * math.sin(2 * math.pi * num / den)
    if im is None:
        return (re * cos, re * sin)
    return (re * cos - im * sin, re * sin + im * cos)


def fix(a):
    if a is not None and a[0] is None:
        return (jnp.zeros_like(a[1]), a[1])
    return a


def fft(items, sign, wanted):
    size = len(items)
    if size == 1:
        return {0: items[0]}
    half = size // 2
    result = {}
    even = sorted({k // 2 for k in wanted if k % 2 == 0})
    odd = sorted({k // 2 for k in wanted if k % 2 == 1})
    if even:
        sub = fft([c_add(items[i], items[i + half]) for i in range(half)], sign, even)
        result.update({2 * k: v for k, v in sub.items()})
    if odd:
        parts = [
            fix(c_turn(c_sub(items[i], items[i + half]), i, size, sign)) for i in range(half)
        ]
        result.update({2 * k + 1: v for k, v in fft(parts, sign, odd).items()})
    return result


class Plan:
    def __init__(self, mag_shape, n_tx, n_ty):
        self.n_ty = n_ty
        self.devices = n = n_tx * n_ty
        self.block_x, self.block_y = mag_shape[1:]
        self.rows = self.block_x // n_ty
        self.len_x, self.len_y = 2 * self.block_x * n_tx, 2 * self.block_y * n_ty
        self.slots = self.len_y // 2 // LANES
        self.residues = 2 * self.slots
        self.near = self.len_y // n // self.residues
        self.group = LANES // self.rows
        self.steps = self.slots // self.group
        self.freq = n * 2 * self.near
        self.pair = math.gcd(4, self.steps)
        self.spread = 2 * n * self.near
        self.split = 4 * n == LANES and self.group == 2
        lane = np.arange(LANES)
        self.lane_slot, self.lane_kappa = lane // self.rows, lane % self.rows
        if self.split:
            fine = LANES // 4
            self.lane_slot = lane // fine % 2
            self.lane_kappa = 2 * (lane % fine) + lane // (2 * fine)

    def y_tables(self):
        k1 = np.arange(LANES)
        spot = np.arange(LANES)
        angle = 2 * np.pi * np.outer(k1, spot) / LANES
        cos, sin = np.cos(angle), np.sin(angle)

        def rows(re_re, re_im, im_re, im_im):
            full = np.stack(
                [np.concatenate([re_re, re_im], 1), np.concatenate([im_re, im_im], 1)]
            )
            full = full.reshape(2, self.devices, self.near, 2 * LANES)
            return full.transpose(1, 0, 2, 3).reshape(self.freq, 2 * LANES)

        plain = rows(cos, sin, -sin, cos)
        mixed = rows(-sin, cos, -cos, -sin)
        slot = np.arange(self.slots)
        turn = 2 * np.pi * np.outer(slot, spot) / self.len_y
        turn_cos = np.tile(np.cos(turn), 2).reshape(self.steps, 1, self.group * 2 * LANES)
        turn_sin = np.tile(np.sin(turn), 2).reshape(self.steps, 1, self.group * 2 * LANES)
        late = 2 * np.pi * np.outer(k1 + 0.5, spot) / LANES
        low = (k1 < LANES // 2)[:, None]
        zero = np.zeros_like(cos)
        im_first = np.where(low, -sin, 0)
        im_first[0] = np.cos(np.pi * spot)
        first = rows(
            np.where(low, cos, zero),
            np.where(low, zero, np.cos(late)),
            im_first,
            np.where(low, zero, -np.sin(late)),
        )
        return plain, mixed, turn_cos, turn_sin, first

    def y_matrices(self):
        plain, mixed, turn_cos, turn_sin, first = (
            jnp.asarray(t, jnp.float32) for t in self.y_tables()
        )
        plain = jnp.concatenate([plain] * self.group, axis=1)[None]
        mixed = jnp.concatenate([mixed] * self.group, axis=1)[None]
        full = plain * turn_cos + mixed * turn_sin
        first = jnp.pad(first, ((0, 0), (0, (self.group - 1) * 2 * LANES)))[None]
        shape = (self.steps, 1, self.group * 2 * LANES)
        at_first = (lax.broadcasted_iota(jnp.int32, shape, 0) == 0) & (
            lax.broadcasted_iota(jnp.int32, shape, 2) < 2 * LANES
        )
        return jnp.where(at_first, first, full)

    def x_first(self):
        n = self.devices
        angle = 2 * np.pi * np.outer(np.arange(2 * n), np.arange(n)) / (2 * n)
        cos, sin = np.cos(angle), np.sin(angle)
        table = np.stack([np.stack([cos, sin], -1), np.stack([-sin, cos], -1)])
        full = np.einsum("orsi,fg->ofrsig", table, np.eye(self.near))
        return full.reshape(2 * self.spread, self.freq)

    def x_turn(self):
        angle = -2 * np.pi * np.outer(np.arange(2 * self.devices), np.arange(self.rows))
        angle = np.tile(angle / self.len_x, (self.near, self.group))
        return np.stack([np.cos(angle), np.sin(angle)]).astype(np.float32)

    def x_second(self):
        span = np.arange(self.rows)
        angle = 2 * np.pi * np.outer(span, span) / self.rows
        cos, sin = np.cos(angle), np.sin(angle)
        table = np.stack([np.stack([cos, -sin], 1), np.stack([sin, cos], 1)])
        full = np.einsum("ixok,qp->iqxopk", table, np.eye(self.group))
        full = full[:, :, :, :, self.lane_slot, self.lane_kappa]
        return full.reshape(2 * LANES, 2 * LANES)


def y_forward_kernel(plan, place_ref, rows_ref, high_ref, low_ref, out_ref, z_high, z_low):
    step = pl.program_id(0)
    chunk = 16
    per = plan.rows // chunk
    blocks = plan.block_y // LANES

    @pl.when(step == 0)
    def _():
        if plan.group > 1:
            z_high[...] = jnp.zeros_like(z_high)
            z_low[...] = jnp.zeros_like(z_low)

        def one(index, carry):
            comp = index // per
            start = pl.multiple_of((index % per) * chunk, chunk)
            items = []
            for block in range(plan.slots):
                lane = block % blocks * LANES
                items.append(
                    (
                        rows_ref[
                            lax.bitwise_xor(block // blocks, place_ref[0]),
                            comp,
                            pl.ds(start, chunk),
                            lane : lane + LANES,
                        ],
                        None,
                    )
                )
            items += [None] * plan.slots
            parts = fft(items, -1, list(range(plan.slots + 1)))
            for slot in range(plan.slots):
                pair = (parts[0][0], parts[plan.slots][0]) if slot == 0 else parts[slot]
                place, inner = slot // plan.group, slot % plan.group
                row = pl.multiple_of(comp * LANES + inner * plan.rows + start, chunk)
                for half in range(2):
                    lane = inner * 2 * LANES + half * LANES
                    high, low = halves(pair[half])
                    z_high[place, pl.ds(row, chunk), lane : lane + LANES] = high
                    z_low[place, pl.ds(row, chunk), lane : lane + LANES] = low
            return carry

        lax.fori_loop(0, rows_ref.shape[1] * per, one, 0)

    wide = z_high.shape[1]
    for part in range(plan.pair):
        place = step * plan.pair + part
        left = (high_ref[part], low_ref[part])
        out_ref[:, part * wide : (part + 1) * wide] = dot_3(
            left, (z_high[place], z_low[place]), NT
        )


def y_forward(plan, place, rows, high, low):
    wide = rows.shape[1] * LANES
    deep = plan.group * 2 * LANES
    matrix = pl.BlockSpec((plan.pair, plan.freq, deep), lambda i: (i, 0, 0))
    return pl.pallas_call(
        functools.partial(y_forward_kernel, plan),
        grid=(plan.steps // plan.pair,),
        in_specs=[
            pl.BlockSpec(memory_space=pltpu.SMEM),
            pl.BlockSpec(rows.shape, lambda i: (0, 0, 0, 0)),
            matrix,
            matrix,
        ],
        out_specs=pl.BlockSpec((plan.freq, plan.pair * wide), lambda i: (0, i)),
        out_shape=jax.ShapeDtypeStruct((plan.freq, wide * plan.steps), jnp.float32),
        scratch_shapes=[
            pltpu.VMEM((plan.steps, wide, deep), jnp.bfloat16),
            pltpu.VMEM((plan.steps, wide, deep), jnp.bfloat16),
        ],
        compiler_params=pltpu.CompilerParams(vmem_limit_bytes=50 * 2**20),
        cost_estimate=pl.CostEstimate(
            flops=6 * plan.freq * wide * plan.steps * deep,
            bytes_accessed=10 * 2**20,
            transcendentals=0,
        ),
        name="y_forward",
    )(place, rows, high, low)


def x_kernel(
    plan,
    data_ref,
    gain_ref,
    shift_ref,
    mirror_ref,
    one_high,
    one_low,
    back_high,
    back_low,
    two_high,
    two_low,
    turn_ref,
    out_ref,
    field_ref,
):
    one = (one_high[...], one_low[...])
    two = (two_high[...], two_low[...])
    turn_re, turn_im = turn_ref[0], turn_ref[1]
    size = plan.spread
    count = field_ref.shape[0]

    def cut(comp):
        return slice(comp * LANES, (comp + 1) * LANES)

    def spectrum(data):
        section = dot_3(one, halves(data))
        result = []
        for comp in range(count):
            re, im = section[:size, cut(comp)], section[size:, cut(comp)]
            turned = jnp.concatenate(
                [re * turn_re - im * turn_im, re * turn_im + im * turn_re], axis=1
            )
            result.append(dot_3(halves(turned), two))
        return result

    def apply(gain, parts):
        wide = [jnp.concatenate([gain(i)] * 2, axis=1) for i in range(2 * count - 1)]
        if count == 1:
            return [wide[0] * parts[0]]
        return [
            wide[0] * parts[0] + wide[2] * parts[1],
            wide[2] * parts[0] + wide[1] * parts[1],
        ]

    data = data_ref[...]
    parts = spectrum(data)
    for comp, value in enumerate(apply(lambda i: gain_ref[i, 0], parts)):
        field_ref[comp] = value

    @pl.when(pl.program_id(0) == 0)
    def _():
        row = lax.broadcasted_iota(jnp.int32, (plan.freq, 1), 0)
        sign = jnp.where(row // plan.near % 2 == 0, 1.0, -1.0)
        other = spectrum(data * sign)
        added = apply(lambda i: shift_ref[i], parts)
        flipped = apply(lambda i: mirror_ref[i], other)
        for comp in range(count):
            field_ref[comp] += added[comp] + flipped[comp]

    re_list, im_list = [], []
    for comp in range(count):
        value = dot_3(halves(field_ref[comp]), two, NT)
        re, im = value[:, :LANES], value[:, LANES:]
        re_list.append(re * turn_re + im * turn_im)
        im_list.append(im * turn_re - re * turn_im)
    section = jnp.concatenate(
        [jnp.concatenate(re_list, axis=1), jnp.concatenate(im_list, axis=1)], axis=0
    )
    out_ref[...] = dot_3((back_high[...], back_low[...]), halves(section))


def x_stage(plan, data, gains, group, tables):
    gain, shift, mirror = gains
    size, index = group
    count = (size + 1) // 2
    wide = count * LANES
    lane_block = pl.BlockSpec((plan.freq, wide), lambda i: (0, i))

    def whole(array):
        return pl.BlockSpec(array.shape, lambda i: (0,) * array.ndim)

    return pl.pallas_call(
        functools.partial(x_kernel, plan),
        grid=(plan.steps,),
        in_specs=[
            lane_block,
            pl.BlockSpec((size, 1, plan.spread, LANES), lambda i: (index, i, 0, 0)),
            pl.BlockSpec((size, plan.spread, LANES), lambda i: (index, 0, 0)),
            pl.BlockSpec((size, plan.spread, LANES), lambda i: (index, 0, 0)),
            *[whole(t) for t in tables],
        ],
        out_specs=lane_block,
        out_shape=jax.ShapeDtypeStruct(data.shape, jnp.float32),
        scratch_shapes=[pltpu.VMEM((count, plan.spread, 2 * LANES), jnp.float32)],
        compiler_params=pltpu.CompilerParams(vmem_limit_bytes=50 * 2**20),
        cost_estimate=pl.CostEstimate(
            flops=24 * plan.freq * wide * plan.steps * 2 * plan.spread,
            bytes_accessed=12 * 2**20,
            transcendentals=0,
        ),
        name="x_stage",
    )(data, gain, shift, mirror, *tables)


def y_inverse_kernel(plan, place_ref, data_ref, high_ref, low_ref, turn_ref, out_ref, inner_ref, sum_ref):
    step = pl.program_id(0)
    deep = 2 * LANES
    lane = lax.broadcasted_iota(jnp.int32, (1, LANES), 1)
    count = out_ref.shape[1]
    wide = count * LANES
    for part in range(plan.pair):
        data = halves(data_ref[:, part * wide : (part + 1) * wide])
        value = dot_3((high_ref[part], low_ref[part]), data)
        for comp in range(count):
            span = slice(comp * LANES, (comp + 1) * LANES)
            mixed = value[:deep, span]
            for inner in range(1, plan.group):
                other = value[inner * deep : (inner + 1) * deep, span]
                mixed = jnp.where(lane // plan.rows == inner, other, mixed)
            inner_ref[comp, step * plan.pair + part] = mixed

    @pl.when(step == plan.steps // plan.pair - 1)
    def _():
        chunk = 16
        blocks = plan.block_y // LANES

        def one_comp(comp, carry):
            def one(index, carry):
                start = pl.multiple_of(index * chunk, chunk)
                items = [
                    (
                        inner_ref[comp, place, pl.ds(start, chunk), :],
                        inner_ref[comp, place, pl.ds(LANES + start, chunk), :],
                    )
                    for place in range(plan.steps)
                ]
                odd = jnp.where(lane < plan.rows, items[0][1], 0.0)
                period = 2 * plan.steps
                parts = fft(items + [None] * plan.steps, 1, list(range(period)))
                for block in range(plan.slots):
                    re, im = parts[block % period]
                    total = re * turn_ref[0, block : block + 1, :]
                    total = total - im * turn_ref[1, block : block + 1, :]
                    total = total + odd if block % 2 == 0 else total - odd
                    shift = LANES // 2
                    while shift >= plan.rows:
                        total = total + pltpu.roll(total, shift, 1)
                        shift //= 2
                    sum_ref[block, pl.ds(start, chunk), :] = total
                return carry

            lax.fori_loop(0, LANES // chunk, one, 0)
            for block in range(plan.slots):
                first = block % blocks * LANES
                target = lax.bitwise_xor(block // blocks, place_ref[0])
                out_ref[target, comp, :, first : first + LANES] = sum_ref[block].T[: plan.rows]
            return carry

        lax.fori_loop(0, count, one_comp, 0)


def y_inverse(plan, place, data, high, low):
    wide = data.shape[1] // plan.steps
    count = wide // LANES
    deep = plan.group * 2 * LANES
    matrix = pl.BlockSpec((plan.pair, deep, plan.freq), lambda i: (i, 0, 0))
    shape = (plan.n_ty, count, plan.rows, plan.block_y)
    inner = np.arange(LANES) // plan.rows
    angle = 2 * np.pi * np.outer(np.arange(plan.slots), inner) / plan.residues
    turn = jnp.asarray(np.stack([np.cos(angle), np.sin(angle)]), jnp.float32)
    return pl.pallas_call(
        functools.partial(y_inverse_kernel, plan),
        grid=(plan.steps // plan.pair,),
        in_specs=[
            pl.BlockSpec(memory_space=pltpu.SMEM),
            pl.BlockSpec((plan.freq, plan.pair * wide), lambda i: (0, i)),
            matrix,
            matrix,
            pl.BlockSpec(turn.shape, lambda i: (0, 0, 0)),
        ],
        out_specs=pl.BlockSpec(shape, lambda i: (0, 0, 0, 0)),
        out_shape=jax.ShapeDtypeStruct(shape, jnp.float32),
        scratch_shapes=[
            pltpu.VMEM((count, plan.steps, 2 * LANES, LANES), jnp.float32),
            pltpu.VMEM((plan.slots, LANES, LANES), jnp.float32),
        ],
        compiler_params=pltpu.CompilerParams(vmem_limit_bytes=50 * 2**20),
        cost_estimate=pl.CostEstimate(
            flops=6 * plan.freq * wide * plan.steps * deep,
            bytes_accessed=10 * 2**20,
            transcendentals=0,
        ),
        name="y_inverse",
    )(place, data, high, low, turn)


ORDER = (0, 1, 3, 2)


def gain_kernel(plan, scale, late_ref, kernel_ref, wave_x_ref, wave_y_ref, out_ref, sort_ref):
    slots = plan.slots
    blocks = plan.len_x // LANES
    row = lax.broadcasted_iota(jnp.int32, (slots, 1), 0)
    lane = lax.broadcasted_iota(jnp.int32, (1, LANES), 1)
    swapped = (row == 0) & (late_ref[0] == 1)
    for block in range(blocks):
        span = slice(block * LANES, (block + 1) * LANES)
        value = kernel_ref[0, :slots, span]
        value = jnp.where(swapped, kernel_ref[0, slots : slots + 1, span], value)
        sort_ref[pl.ds(block, slots, stride=blocks), :] = value
    diagonal = jnp.where(pl.program_id(0) == 2, 0.0, scale)
    half = LANES // 2
    for pair in range(plan.steps // 2):
        turned = sort_ref[pair * LANES : (pair + 1) * LANES, :].T
        low, high = turned[:half], turned[half:]
        parts = (
            jnp.where(lane < half, low, pltpu.roll(high, half, 1)),
            jnp.where(lane < half, pltpu.roll(low, half, 1), high),
        )
        for i, part in enumerate(parts):
            step = 2 * pair + i
            wave = wave_x_ref[...] + wave_y_ref[0, step : step + 1, :]
            out_ref[0, step] = diagonal * wave - scale * part


def kernel_gains(plan, kernel):
    n, near, slots = plan.devices, plan.near, plan.slots
    me = lax.axis_index(AXES)
    scale = 2.0 / (plan.len_x * plan.len_y)
    r = np.arange(2 * n)
    kx = 2 * n * plan.lane_kappa[None] + r[:, None]
    wave_x = jnp.asarray(2 * STIFFNESS * np.cos(2 * np.pi * kx / plan.len_x), jnp.float32)
    late = me >= n // 2
    slot = lax.broadcasted_iota(jnp.int32, (near, slots), 1)
    slot = jnp.where((slot == 0) & late, slots, slot)
    ky = (me * near + lax.broadcasted_iota(jnp.int32, (near, slots), 0)) * plan.residues + slot
    wave_y = 2 * STIFFNESS * jnp.cos(ky.astype(jnp.float32) * (2 * math.pi / plan.len_y))
    wave_y = wave_y.reshape(near, plan.steps, plan.group)
    wave_y = sum(
        wave_y[:, :, i : i + 1] * jnp.asarray(plan.lane_slot == i, jnp.float32)
        for i in range(plan.group)
    )
    if plan.split:
        out_shape = (4, plan.steps, plan.spread, LANES)
        gain = pl.pallas_call(
            functools.partial(gain_kernel, plan, scale),
            grid=(4, near),
            in_specs=[
                pl.BlockSpec(memory_space=pltpu.SMEM),
                pl.BlockSpec(
                    (1, plan.residues, plan.len_x),
                    lambda c, f: (jnp.where(c < 2, c, 5 - c), f, 0),
                ),
                pl.BlockSpec(wave_x.shape, lambda c, f: (0, 0)),
                pl.BlockSpec((1, plan.steps, LANES), lambda c, f: (f, 0, 0)),
            ],
            out_specs=pl.BlockSpec((1, plan.steps, 2 * n, LANES), lambda c, f: (c, 0, f, 0)),
            out_shape=jax.ShapeDtypeStruct(out_shape, jnp.float32),
            scratch_shapes=[pltpu.VMEM((slots * plan.len_x // LANES, LANES), jnp.float32)],
            compiler_params=pltpu.CompilerParams(vmem_limit_bytes=16 * 2**20),
            cost_estimate=pl.CostEstimate(
                flops=2**30, bytes_accessed=12 * 2**20, transcendentals=0
            ),
            name="gain",
        )(late.astype(jnp.int32).reshape(1), kernel, wave_x, wave_y)
    else:
        kernel_4 = kernel.reshape(4, near, plan.residues, plan.len_x)
        first = jnp.where(late, kernel_4[:, :, slots : slots + 1], kernel_4[:, :, :1])
        chosen = jnp.concatenate([first, kernel_4[:, :, 1:slots]], axis=2)
        shaped = chosen.reshape(4, near, plan.steps, plan.group, plan.rows, 2 * n)
        moved = shaped.transpose(0, 2, 1, 5, 3, 4).reshape(4, plan.steps, near, 2 * n, LANES)
        moved = jnp.stack([moved[i] for i in ORDER])
        wave = wave_x + wave_y.transpose(1, 0, 2)[:, :, None]
        gain = jnp.concatenate([wave[None] - moved[:2], -moved[2:3], wave[None] - moved[3:]])
        gain = (scale * gain).reshape(4, plan.steps, plan.spread, LANES)

    nyquist = lax.ppermute(kernel[:, 0, :], AXES, [(n // 2, 0)])

    def arrange(row, wave_y):
        row = jnp.stack([row[i] for i in ORDER])
        if plan.split:
            small = row.reshape(4, plan.rows // 2, 2, 2 * n).transpose(0, 3, 2, 1)
        else:
            small = row.reshape(4, plan.rows, 1, 2 * n).transpose(0, 3, 2, 1)
        small = jnp.pad(small[:, :, :, None], ((0, 0),) * 3 + ((0, plan.group - 1), (0, 0)))
        small = small.reshape(4, 2 * n, LANES)
        diagonal = jnp.asarray([1.0, 1.0, 0.0, 1.0], jnp.float32)[:, None, None]
        return (diagonal * (wave_x + wave_y) - small) * scale

    zero_row = arrange(kernel[:, 0, :], 2 * STIFFNESS)
    last_row = arrange(nyquist, -2 * STIFFNESS)
    used = jnp.asarray(plan.lane_slot == 0) & (me == 0)

    def place(rows):
        rows = jnp.where(used, rows, 0.0)[:, None]
        rows = jnp.pad(rows, ((0, 0), (0, near - 1), (0, 0), (0, 0)))
        return rows.reshape(4, plan.spread, LANES)

    shift = place(0.25 * (zero_row + last_row) - zero_row)
    return gain, shift, place(0.25 * (zero_row - last_row))


def cross(left, right):
    return [
        left[1] * right[2] - left[2] * right[1],
        left[2] * right[0] - left[0] * right[2],
        left[0] * right[1] - left[1] * right[0],
    ]


def inner(left, right):
    return left[0] * right[0] + left[1] * right[1] + left[2] * right[2]


def rate(field, effective):
    torque = cross(field, effective)
    again = cross(field, torque)
    return [-(t + DAMPING * a) / (1.0 + DAMPING * DAMPING) for t, a in zip(torque, again)]


def normal(vector, occ):
    size = jnp.sqrt(inner(vector, vector) + 1.0 - occ)
    return [v / size for v in vector]


def swap(values, axis, offset):
    size = lax.axis_size(axis)
    return lax.ppermute(values, axis, [(i, i ^ offset) for i in range(size)])


def exchange(values, axes):
    return lax.all_to_all(values, axes, split_axis=0, concat_axis=0, tiled=True)


def body(mag, occupancy, kernel_spectrum):
    plan = Plan(mag.shape, lax.axis_size("tx"), lax.axis_size("ty"))
    occ = occupancy.astype(jnp.float32)
    start = mag * occ[None]
    matrix = plan.y_matrices()
    rounded = lax.reduce_precision(matrix, 8, 7)
    high, low = rounded.astype(jnp.bfloat16), (matrix - rounded).astype(jnp.bfloat16)
    high_back, low_back = jnp.swapaxes(high, 1, 2), jnp.swapaxes(low, 1, 2)
    one = plan.x_first()
    tables = (
        *np_halves(one),
        *np_halves(one.T),
        *np_halves(plan.x_second()),
        jnp.asarray(plan.x_turn()),
    )
    gains = kernel_gains(plan, kernel_spectrum)

    def sent(array):
        return array.reshape(plan.devices, 2 * plan.near, array.shape[1])

    def flat(array):
        return array.reshape(plan.freq, array.shape[2])

    here = lax.axis_index("ty")
    place = here.reshape(1)

    def start_row(offset):
        return (here ^ offset) * plan.rows

    def gather_rows(field):
        size = (field.shape[0], plan.rows, plan.block_y)
        pieces = []
        for offset in range(plan.n_ty):
            piece = lax.dynamic_slice(field, (0, start_row(offset), 0), size)
            pieces.append(swap(piece, "ty", offset) if offset else piece)
        return jnp.stack(pieces)

    def return_rows(spatial):
        count = spatial.shape[1]
        field = jnp.zeros((count, plan.block_x, plan.block_y), jnp.float32)
        for offset in range(plan.n_ty):
            piece = swap(spatial[offset], "ty", offset) if offset else spatial[0]
            field = lax.dynamic_update_slice(field, piece, (0, start_row(offset), 0))
        return field

    def effective(rows_a, rows_b):
        spectra_a = sent(y_forward(plan, place, rows_a, high, low))
        columns_a = exchange(spectra_a, AXES)
        spectra_b = sent(y_forward(plan, place, rows_b, high, low))
        columns_a, spectra_b = lax.optimization_barrier((columns_a, spectra_b))
        columns_b = exchange(spectra_b, AXES)
        product_a = sent(x_stage(plan, flat(columns_a), gains, (1, 3), tables))
        product_a, columns_b = lax.optimization_barrier((product_a, columns_b))
        returned_a = exchange(product_a, AXES)
        product_b = sent(x_stage(plan, flat(columns_b), gains, (3, 0), tables))
        returned_a, product_b = lax.optimization_barrier((returned_a, product_b))
        returned_b = exchange(product_b, AXES)
        field_a = y_inverse(plan, place, flat(returned_a), high_back, low_back)
        field_b = y_inverse(plan, place, flat(returned_b), high_back, low_back)
        return [field_b[:, 0], field_b[:, 1], field_a[:, 0]]

    rows_a = gather_rows(start[2:])
    rows_b = gather_rows(start[:2])
    field = effective(rows_a, rows_b)
    begin = [rows_b[:, 0], rows_b[:, 1], rows_a[:, 0]]
    held = jnp.where(inner(begin, begin) > 0.25, 1.0, 0.0)
    first = rate(begin, field)
    middle = normal([b + TIME_STEP * f for b, f in zip(begin, first)], held)
    field = effective(middle[2][:, None], jnp.stack(middle[:2], axis=1))
    second = rate(middle, field)
    along = inner(second, begin)
    mean = [0.5 * (f + (s - along * b)) for f, s, b in zip(first, second, begin)]
    mean_rate = return_rows(jnp.stack(mean, axis=1))
    moved = start + TIME_STEP * mean_rate
    return (jnp.stack(normal([moved[0], moved[1], moved[2]], occ)), mean_rate)


def solution(mesh):
    return jax.shard_map(
        body,
        mesh=mesh,
        in_specs=(P(None, "tx", "ty"), P("tx", "ty"), P(None, ("tx", "ty"), None)),
        out_specs=(P(None, "tx", "ty"), P(None, "tx", "ty")),
        check_vma=False,
    )
```
